32 devices in a mesh: seq: 16 (over z, y, core), batch: 2 (over x).
Axes of the slice: x: 2, y: 2, z: 4, core: 2. Of those that a mesh axis runs over, the one named last changes fastest.
Arguments:
- queries: bfloat16 [4096, 1792], P(('batch', 'seq')), parts along dimension 0, may hold values from -128 to 128
- keys: bfloat16 [4096, 256], P(('batch', 'seq')), parts along dimension 0, may hold values from -4 to 4
- values: bfloat16 [4096, 256], P(('batch', 'seq')), parts along dimension 0, may hold values from -4 to 4
- out_grad: bfloat16 [4096, 1792], P(('batch', 'seq')), parts along dimension 0, may hold values from -24 to 24
- row_delta: float32 [4096, 14], P(('batch', 'seq')), parts along dimension 0, may hold values from -6 to 6
- layer_input: bfloat16 [4096, 3584], P(('batch', 'seq')), parts along dimension 0, may hold values from -6 to 6
- norm_gain: float32 [3584], replicated, may hold values from 0.25 to 1.75
- qkv_weight: bfloat16 [3584, 2304], P('seq'), may hold values from -0.5 to 0.5
- block_order: int32 [64], P('batch'), parts along dimension 0, may hold values from 0 to 31, as said below
- block_mask: int32 [64, 32], P('batch'), parts along dimension 0, may hold values from 0 to 1, as said below
- frame_owner: int32 [32], P('batch'), parts along dimension 0, may hold values from 0 to 15, as said below
- vision_features: bfloat16 [32, 128, 1152], P(('batch', 'seq')), parts along dimension 0, may hold values from -6 to 6
- post_gain: float32 [1152], replicated, may hold values from 0.25 to 1.75
- projector: bfloat16 [1152, 3584], replicated, may hold values from -0.1875 to 0.1875
Outputs:
- token_grad: bfloat16 [4096, 3584], P(('batch', 'seq')), parts along dimension 0
- encoder_grad: bfloat16 [32, 128, 1152], P(('batch', 'seq')), parts along dimension 0
The draws below stay inside these ranges and needn't reach their ends.
There are 2 independent parts, one for each index of `batch`. The reference program is written for one: setup_inputs(seed, part) draws one part's arguments, and reference() takes and returns one part's arrays. A program takes and returns all parts, laid end to end along the dimension named above; an argument that names none is the same for every part. Nothing has to cross between parts.
Inputs may be any that keep to these rules, and one draw needn't show every extreme that they name: `block_order`: entries 2i and 2i + 1 are the blocks of device i of seq; all entries together are a permutation; each device's two blocks sum to 31; for every frame f, blocks 2f and 2f + 1 lie on devices 2j and 2j + 1 for some j. `block_mask`: 1 on the diagonal, 0 above it. `frame_owner`: every device of seq owns exactly one frame, and the owner of frame f holds block 2f or block 2f + 1.
All inputs are finite; a program needn't handle non-finite values.
Results may differ from the reference program's by a relative error of at most 0.012.
Values may be sent and summed in bfloat16 or wider, within the bound.
A program may use at most 128 MiB of HBM per device.

```python
import jax
import jax.numpy as jnp
from jax import lax

D = 3584
HQ = 14
KVH = 2
HD = 128
C_ENC = 1152
TOK_DEV = 128
QKV = 2304
SEQ_LEN = 2048
FRAMES = 16
N_SEQ = 16


def frame_layout(key):
    count = N_SEQ
    groups = count // 2
    slot = jax.random.permutation(jax.random.fold_in(key, 11), groups).astype(jnp.int32)
    flip = jax.random.randint(jax.random.fold_in(key, 12), (groups,), 0, 2).astype(jnp.int32)
    order_first = jax.random.randint(jax.random.fold_in(key, 13), (groups,), 0, 2).astype(jnp.int32)
    order_second = jax.random.randint(jax.random.fold_in(key, 14), (groups,), 0, 2).astype(jnp.int32)
    owner_bit = jax.random.randint(jax.random.fold_in(key, 15), (groups,), 0, 2).astype(jnp.int32)
    group_ids = jnp.arange(groups, dtype=jnp.int32)
    device_first = (2 * slot + flip).astype(jnp.int32)
    device_second = (2 * slot + 1 - flip).astype(jnp.int32)
    first_lead = jnp.where(order_first == 1, 2 * count - 1 - 2 * group_ids, 2 * group_ids).astype(jnp.int32)
    second_lead = jnp.where(order_second == 1, 2 * count - 2 - 2 * group_ids, 2 * group_ids + 1).astype(jnp.int32)
    order = jnp.zeros((2 * count,), jnp.int32)
    order = order.at[2 * device_first].set(first_lead).at[2 * device_first + 1].set(2 * count - 1 - first_lead)
    order = order.at[2 * device_second].set(second_lead).at[2 * device_second + 1].set(2 * count - 1 - second_lead)
    owner = jnp.zeros((count,), jnp.int32)
    owner = owner.at[group_ids].set(jnp.where(owner_bit == 1, device_second, device_first))
    owner = owner.at[count - 1 - group_ids].set(jnp.where(owner_bit == 1, device_first, device_second))
    return (order.astype(jnp.int32), owner.astype(jnp.int32))


def draw_block_order(key, part):
    return frame_layout(key)[0]


def draw_frame_owner(key, part):
    return frame_layout(key)[1]


def draw_block_mask(key, part):
    count_blocks = 2 * N_SEQ
    random_bits = jax.random.randint(jax.random.fold_in(key, 21), (count_blocks, count_blocks), 0, 2).astype(jnp.int32)
    row_index = jnp.arange(count_blocks, dtype=jnp.int32)[:, None]
    column_index = jnp.arange(count_blocks, dtype=jnp.int32)[None, :]
    return jnp.where(row_index > column_index, random_bits, jnp.where(row_index == column_index, 1, 0)).astype(jnp.int32)


def attention_inputs(key):
    total_rows = TOK_DEV * N_SEQ
    half_len = TOK_DEV // 2
    group_size = HQ // KVH
    count_blocks = 2 * N_SEQ
    ranking = jnp.stack([jax.random.permutation(jax.random.fold_in(key, 40 + head), HD) for head in range(KVH)]).astype(jnp.int32)
    dim_scale = jnp.where(ranking < HD // 2, 1.5, 0.5).astype(jnp.float32)
    block_scale = jnp.exp(jax.random.uniform(jax.random.fold_in(key, 41), (count_blocks, 1, KVH, HD), jnp.float32, jnp.log(0.7), jnp.log(1.4)))
    key_scale = dim_scale[None, None, :, :] * block_scale
    limit = 4.0 / key_scale
    key_base = jax.random.truncated_normal(jax.random.fold_in(key, 31), -limit, limit, (count_blocks, half_len, KVH, HD), jnp.float32)
    keys_drawn = (key_base * key_scale).reshape(total_rows, KVH, HD)
    query_base = jax.random.truncated_normal(jax.random.fold_in(key, 32), -4.0, 4.0, (total_rows, KVH, group_size, HD), jnp.float32)
    queries_drawn = query_base * dim_scale[None, :, None, :]
    return (queries_drawn.reshape(total_rows, HQ * HD), keys_drawn.reshape(total_rows, KVH * HD))


def draw_queries(key, part):
    return attention_inputs(key)[0].astype(jnp.bfloat16)


def draw_keys(key, part):
    return attention_inputs(key)[1].astype(jnp.bfloat16)


def level_of(key, extent, cuts, smallest, largest):
    factor_of, own = 1.0, jax.random.fold_in(key, 6)
    for dim, shards_of in cuts:
        heights = jnp.exp(jax.random.uniform(jax.random.fold_in(own, dim), (shards_of,), jnp.float32, smallest / len(cuts), largest / len(cuts)))
        factor_of = factor_of * jnp.repeat(heights, extent[dim] // shards_of).reshape([-1 if axis == dim else 1 for axis in range(len(extent))])
    return factor_of


def gaussian(key, dims, scale, most, cuts=(), held_as=jnp.bfloat16):
    values = jax.random.normal(key, dims, jnp.float32) * scale
    if len(cuts) > 0:
        values = level_of(key, dims, cuts, -0.22, 0.18) * values
    return jnp.clip(values, min=-most, max=most).astype(held_as)


def setup_inputs(seed: int = 0, part: int = 0) -> dict:
    key_of = jax.random.split(jax.random.key(seed), 15)
    part_splits = jax.random.split(jax.random.fold_in(key_of[14], part), 15)
    return {
        "queries": draw_queries(jax.random.fold_in(jax.random.fold_in(key_of[14], part), 71), part),
        "keys": draw_keys(jax.random.fold_in(jax.random.fold_in(key_of[14], part), 71), part),
        "values": gaussian(part_splits[2], (SEQ_LEN, KVH * HD), 1.0, 4.0, ((0, 16),)),
        "out_grad": gaussian(part_splits[3], (SEQ_LEN, HQ * HD), 4.0, 24.0, ((0, 16),)),
        "row_delta": gaussian(part_splits[4], (SEQ_LEN, HQ), 1.0, 6.0, ((0, 16),), jnp.float32),
        "layer_input": gaussian(part_splits[5], (SEQ_LEN, D), 1.0, 6.0, ((0, 16),)),
        "norm_gain": jnp.clip(1.0 + 0.15 * jax.random.normal(key_of[6], (D,), jnp.float32), 0.25, 1.75),
        "qkv_weight": gaussian(key_of[7], (D, QKV), HD ** -0.5, 0.5, ((0, 16),)),
        "block_order": draw_block_order(jax.random.fold_in(jax.random.fold_in(key_of[14], part), 71), part),
        "block_mask": draw_block_mask(jax.random.fold_in(jax.random.fold_in(key_of[14], part), 71), part),
        "frame_owner": draw_frame_owner(jax.random.fold_in(jax.random.fold_in(key_of[14], part), 71), part),
        "vision_features": gaussian(part_splits[11], (FRAMES, TOK_DEV, C_ENC), 1.0, 6.0, ((0, 16),)),
        "post_gain": jnp.clip(1.0 + 0.15 * jax.random.normal(key_of[12], (C_ENC,), jnp.float32), 0.25, 1.75),
        "projector": gaussian(key_of[13], (C_ENC, D), C_ENC ** -0.5, 0.1875),
    }


EPSILON = 1e-06
NEGATIVE = -1e+30

def reference(queries, keys, values, out_grad, row_delta, layer_input, norm_gain, qkv_weight, block_order, block_mask, frame_owner, vision_features, post_gain, projector):
    half_len = TOK_DEV // 2
    total_rows = TOK_DEV * N_SEQ
    group_size = HQ // KVH
    scaling = HD ** (-0.5)
    row_ids = jnp.arange(total_rows, dtype=jnp.int32)
    position = (block_order[row_ids // half_len] * half_len + row_ids % half_len).astype(jnp.int32)
    blocks = (position // half_len).astype(jnp.int32)
    query_heads = queries.reshape(total_rows, HQ, HD)
    grad_heads = out_grad.reshape(total_rows, HQ, HD)
    key_heads = keys.reshape(total_rows, KVH, HD)
    value_heads = values.reshape(total_rows, KVH, HD)

    def one_head(head_index):
        kv_index = (head_index // group_size).astype(jnp.int32)
        query_rows = lax.dynamic_index_in_dim(query_heads, head_index, 1, keepdims=False)
        grad_rows = lax.dynamic_index_in_dim(grad_heads, head_index, 1, keepdims=False)
        key_rows = lax.dynamic_index_in_dim(key_heads, kv_index, 1, keepdims=False)
        value_rows = lax.dynamic_index_in_dim(value_heads, kv_index, 1, keepdims=False)
        delta_rows = lax.dynamic_index_in_dim(row_delta, head_index, 1, keepdims=False)

        def per_block(running, block_start):
            key_acc, value_acc = running
            query_block = lax.dynamic_slice_in_dim(query_rows, block_start, TOK_DEV, 0)
            grad_block = lax.dynamic_slice_in_dim(grad_rows, block_start, TOK_DEV, 0)
            delta_block = lax.dynamic_slice_in_dim(delta_rows, block_start, TOK_DEV, 0)
            pos_block = lax.dynamic_slice_in_dim(position, block_start, TOK_DEV, 0)
            block_ids = lax.dynamic_slice_in_dim(blocks, block_start, TOK_DEV, 0)
            allowed = (block_mask[block_ids][:, blocks] == 1) & (position[None, :] <= pos_block[:, None])
            score = jnp.dot(query_block, key_rows.T, preferred_element_type=jnp.float32) * scaling
            top_score = lax.optimization_barrier(jnp.max(jnp.where(allowed, score, NEGATIVE), axis=1))
            total_exp = lax.optimization_barrier(jnp.sum(jnp.where(allowed, jnp.exp(score - top_score[:, None]), 0.0), axis=1))
            lse = top_score + jnp.log(total_exp)
            prob = jnp.where(allowed, jnp.exp(score - lse[:, None]), 0.0)
            prob_low = prob.astype(jnp.bfloat16)
            value_acc = value_acc + jnp.dot(prob_low.T, grad_block, preferred_element_type=jnp.float32)
            prob_grad = jnp.dot(grad_block, value_rows.T, preferred_element_type=jnp.float32)
            score_grad = (prob * (prob_grad - delta_block[:, None])).astype(jnp.bfloat16)
            query_out = jnp.dot(score_grad, key_rows, preferred_element_type=jnp.float32) * scaling
            key_acc = key_acc + jnp.dot(score_grad.T, query_block, preferred_element_type=jnp.float32)
            return ((key_acc, value_acc), query_out)
        starting = (jnp.zeros((total_rows, HD), jnp.float32), jnp.zeros((total_rows, HD), jnp.float32))
        starts = (jnp.arange(N_SEQ, dtype=jnp.int32) * TOK_DEV).astype(jnp.int32)
        finals, query_parts = lax.scan(per_block, starting, starts)
        return (query_parts.reshape(total_rows, HD), finals[0] * scaling, finals[1])
    query_all, key_all, value_all = lax.map(one_head, jnp.arange(HQ, dtype=jnp.int32))
    query_grad = jnp.transpose(query_all, (1, 0, 2)).reshape(total_rows, HQ * HD)
    key_grad = jnp.transpose(lax.optimization_barrier(jnp.sum(key_all.reshape(KVH, group_size, total_rows, HD), axis=1)), (1, 0, 2)).reshape(total_rows, KVH * HD)
    value_grad = jnp.transpose(lax.optimization_barrier(jnp.sum(value_all.reshape(KVH, group_size, total_rows, HD), axis=1)), (1, 0, 2)).reshape(total_rows, KVH * HD)
    head_grads = jnp.concatenate([query_grad, key_grad, value_grad], axis=1).astype(jnp.bfloat16)
    norm_grad = jnp.dot(head_grads, qkv_weight.T, preferred_element_type=jnp.float32).astype(jnp.bfloat16)
    inputs = layer_input.astype(jnp.float32)
    inverse = lax.rsqrt(lax.optimization_barrier(jnp.mean(inputs * inputs, axis=1, keepdims=True)) + EPSILON)
    scaled = norm_grad.astype(jnp.float32) * norm_gain
    token_grad = (inverse * scaled - inputs * inverse ** 3 * lax.optimization_barrier(jnp.mean(scaled * inputs, axis=1, keepdims=True))).astype(jnp.bfloat16)
    row_of_position = jnp.zeros((total_rows,), jnp.int32).at[position].set(row_ids)
    device_ids = jnp.arange(N_SEQ, dtype=jnp.int32)
    frame_of_device = jnp.zeros((N_SEQ,), jnp.int32).at[frame_owner].set(device_ids)
    spatial = jnp.arange(TOK_DEV, dtype=jnp.int32)
    frame_rows = row_of_position[(frame_of_device[:, None] * TOK_DEV + spatial[None, :]).astype(jnp.int32)]
    frame_grad = token_grad[frame_rows]
    post_grad = jnp.dot(frame_grad.reshape(N_SEQ * TOK_DEV, D), projector.T, preferred_element_type=jnp.float32).reshape(N_SEQ, TOK_DEV, C_ENC)
    features = vision_features.astype(jnp.float32)
    centered = features - lax.optimization_barrier(jnp.mean(features, axis=2, keepdims=True))
    deviation = lax.rsqrt(lax.optimization_barrier(jnp.mean(centered * centered, axis=2, keepdims=True)) + EPSILON)
    normed = centered * deviation
    weighted = post_grad * post_gain
    encoder_grad = (deviation * (weighted - lax.optimization_barrier(jnp.mean(weighted, axis=2, keepdims=True)) - normed * lax.optimization_barrier(jnp.mean(weighted * normed, axis=2, keepdims=True)))).astype(jnp.bfloat16)
    return (token_grad, encoder_grad)
```

```python
import functools

import jax
import jax.numpy as jnp
from jax import lax
from jax.experimental import pallas as pl
from jax.experimental.pallas import tpu as pltpu
from jax.sharding import PartitionSpec as P

HQ = 14
KVH = 2
HD = 128
GROUP = HQ // KVH
WIDE = GROUP * HD
LOG2E = 1.4426950408889634
EPSILON = 1e-06
NEGATIVE = -1e30
PIECES = 3
MESH = pl.DeviceIdType.MESH


def when(condition, action):
    if condition is None:
        action()
    else:
        pl.when(condition)(action)


def split_rows(size, count):
    tiles = size // 16
    edges = [tiles * i // count for i in range(count + 1)]
    return [(16 * a, 16 * (b - a)) for a, b in zip(edges, edges[1:]) if b > a]


class Copies:
    def __init__(self, send_sem, recv_sem):
        self.send_sem, self.recv_sem = send_sem, recv_sem
        self.sends, self.recvs = 0, 0
        self.started = []

    def slots(self, count=1):
        self.recvs += count
        return self.recvs - count

    def send(self, src, dst, recv, device, condition=None):
        copy = pltpu.make_async_remote_copy(
            src_ref=src,
            dst_ref=dst,
            send_sem=self.send_sem.at[self.sends],
            recv_sem=self.recv_sem.at[recv],
            device_id=device,
            device_id_type=MESH,
        )
        self.sends += 1
        when(condition, copy.start)
        self.started.append((condition, copy))

    def wait(self, ref, recv, device, condition=None):
        copy = pltpu.make_async_remote_copy(
            src_ref=ref,
            dst_ref=ref,
            send_sem=self.send_sem.at[0],
            recv_sem=self.recv_sem.at[recv],
            device_id=device,
            device_id_type=MESH,
        )
        when(condition, copy.wait_recv)

    def drain(self):
        for condition, copy in self.started:
            when(condition, copy.wait_send)


def layer_kernel(
    depth,
    order_ref,
    mask_ref,
    queries_ref,
    grads_ref,
    delta_hbm,
    keys_ref,
    values_ref,
    weight_ref,
    out_ref,
    k_all,
    v_all,
    q_in,
    g_in,
    d_in,
    w_all,
    k_sort,
    v_sort,
    q_sort,
    g_sort,
    d_sort,
    d_pad,
    scores,
    top,
    total,
    dq_acc,
    acc,
    part,
    core_in,
    sum_out,
    z_in,
    h_q,
    h_kv,
    y_out,
    y_in,
    load_sem,
    send_sem,
    recv_sem,
):
    me = lax.axis_index("seq")
    batch = lax.axis_index("batch")
    x = lax.rem(batch, 2)
    z, y, c = me // 4, lax.rem(me // 2, 2), lax.rem(me, 2)
    rows = q_in.shape[1]
    half = rows // 2
    lanes = 2 * GROUP * half
    shard = weight_ref.shape[0]
    scaling = HD ** (-0.5)
    factor = scaling * LOG2E

    up, down = {"seq": me + 4}, {"seq": me - 4}
    beside, core = {"seq": me + 2 - 4 * y}, {"seq": me + 1 - 2 * c}
    corner = {"seq": me + 2 - 4 * y + 1 - 2 * c}
    across = {"batch": batch + 1 - 2 * x}
    has_up, has_down = z < depth - 1, z > 0

    def far(k):
        return lax.rem(z + k, depth)

    def behind(k):
        return lax.rem(z + depth - k, depth)

    def plane(j):
        return {"seq": 4 * j + 2 * y + c}

    def head_at(ref, side, width):
        return ref.at[:, pl.ds(pl.multiple_of(side * width, 128), width)]

    def load(src, dst, index):
        copy = pltpu.make_async_copy(src, dst, load_sem.at[index])
        copy.start()
        return copy

    load_k = load(head_at(keys_ref, y, HD), k_all.at[z, c, y], 0)
    load_v = load(head_at(values_ref, y, HD), v_all.at[z, c, y], 1)
    load_w = load(weight_ref, w_all.at[z], 2)
    load_q = load(head_at(queries_ref, y, WIDE), q_in.at[y], 3)
    load_g = load(head_at(grads_ref, y, WIDE), g_in.at[y], 4)
    load_d = load(delta_hbm, d_in.at[y], 5)

    barrier = pltpu.get_barrier_semaphore()
    peers = [beside, core, corner, across] + [plane(far(k)) for k in range(1, depth)]
    for peer in peers:
        pl.semaphore_signal(barrier, inc=1, device_id=peer, device_id_type=MESH)
    pl.semaphore_wait(barrier, len(peers))

    copies = Copies(send_sem, recv_sem)

    over_y = copies.slots(5)
    copies.send(head_at(keys_ref, 1 - y, HD), k_all.at[z, c, y], over_y, beside)
    copies.send(head_at(values_ref, 1 - y, HD), v_all.at[z, c, y], over_y + 1, beside)
    copies.send(head_at(queries_ref, 1 - y, WIDE), q_in.at[y], over_y + 2, beside)
    copies.send(head_at(grads_ref, 1 - y, WIDE), g_in.at[y], over_y + 3, beside)
    copies.send(delta_hbm, d_in.at[y], over_y + 4, beside)

    def spread(ref, load_own, swap):
        arrive = copies.slots(2 * depth)
        shared = copies.slots(2)

        def own(side, index):
            for k in range(depth - 1, 0, -1):
                copies.send(
                    ref.at[z, c, side], ref.at[z, c, side], arrive + 2 * k + index, plane(far(k))
                )
            copies.send(ref.at[z, c, side], ref.at[z, c, side], shared + index, core)

        def first():
            load_own.wait()
            own(y, 0)

        def second():
            copies.wait(ref.at[z, c, 1 - y], swap, beside)
            own(1 - y, 1)

        passed = copies.slots(depth)

        def relay():
            for k in range(1, depth):
                j = behind(k)
                for index in range(2):
                    side = y if index == 0 else 1 - y
                    copies.wait(ref.at[j, c, side], arrive + 2 * k + index, core)
                copies.send(ref.at[j, c], ref.at[j, c], passed + k, core)

        def finish():
            for index in range(2):
                side = y if index == 0 else 1 - y
                copies.wait(ref.at[z, 1 - c, side], shared + index, core)
            for k in range(1, depth):
                copies.wait(ref.at[behind(k), 1 - c], passed + k, core)

        return first, second, relay, finish

    k_first, k_second, k_relay, k_finish = spread(k_all, load_k, over_y)
    v_first, v_second, v_relay, v_finish = spread(v_all, load_v, over_y + 1)
    k_first()
    k_second()
    v_first()
    v_second()

    own_part = shard // 32 * 16
    between = shard - 2 * own_part
    pieces = split_rows(own_part, PIECES)

    def w_at(j, side, start, size):
        base = pl.multiple_of(side * (shard - own_part) + start, 16)
        return w_all.at[j, pl.ds(base, size)]

    def w_middle(j):
        return w_all.at[j, pl.ds(own_part, between)]

    count = len(pieces)
    w_recv = [copies.slots(depth) for _ in range(count + 1)]
    w_cross = [copies.slots(depth) for _ in range(count)]

    def w_send(j, upward, downward):
        for i in range(count + (between > 0)):
            ref = w_at(j, x, *pieces[i]) if i < count else w_middle(j)
            if upward is not None:
                copies.send(ref, ref, w_recv[i] + j, up, upward)
            if downward is not None:
                copies.send(ref, ref, w_recv[i] + j, down, downward)

    def w_relay(step):
        for j, present, upward in (
            (z - step, z - step >= 0, True),
            (z + step, z + step < depth, False),
        ):
            at = jnp.clip(j, 0, depth - 1)
            go = jnp.logical_and(present, has_up if upward else has_down)
            for i in range(count + (between > 0)):
                ref = w_at(at, x, *pieces[i]) if i < count else w_middle(at)
                copies.wait(ref, w_recv[i] + at, core, present)
                copies.send(ref, ref, w_recv[i] + at, up if upward else down, go)
                if i < count:
                    copies.send(ref, ref, w_cross[i] + at, across, present)

    def w_finish(j, other):
        for i in range(count):
            copies.wait(w_at(j, 1 - x, *pieces[i]), w_cross[i] + j, across, other)

    load_w.wait()
    w_send(z, has_up, has_down)

    def turned(device):
        return order_ref[2 * device] > order_ref[2 * device + 1]

    def arrange(source, target, side):
        flip = turned(4 * z + 2 * side + c)
        for h in range(GROUP):
            first = source[side, 0:half, h * HD : (h + 1) * HD]
            second = source[side, half:rows, h * HD : (h + 1) * HD]
            at = (side * GROUP + h) * half
            target[0, at : at + half] = jnp.where(flip, second, first)
            target[1, at : at + half] = jnp.where(flip, first, second)

    for copy in (load_q, load_g, load_d):
        copy.wait()
    k_relay()
    copies.wait(q_in.at[1 - y], over_y + 2, beside)
    for side in range(2):
        arrange(q_in, q_sort, side)

    def sort_keys(source, target):
        def one(index, carry):
            j, device = index // 4, lax.rem(index, 4)
            owner, side = device // 2, lax.rem(device, 2)
            flip = turned(4 * j + 2 * side + owner)
            first = source[j, owner, side, 0:half]
            second = source[j, owner, side, half:rows]
            at = pl.ds(pl.multiple_of(device * half, half), half)
            target[0, j, at] = jnp.where(flip, second, first)
            target[1, j, at] = jnp.where(flip, first, second)
            return carry

        lax.fori_loop(0, 4 * depth, one, 0)

    k_finish()
    sort_keys(k_all, k_sort)

    tiles = 3 * depth
    lane = lax.broadcasted_iota(jnp.int32, (1, lanes), 1)
    query_row = lax.rem(lane, half)
    in_first = lane < GROUP * half
    key_row = lax.broadcasted_iota(jnp.int32, (half, lanes), 0)

    def block_of(device, high):
        one, two = order_ref[2 * device], order_ref[2 * device + 1]
        return jnp.where(high == 1, jnp.maximum(one, two), jnp.minimum(one, two))

    def tile(t):
        kind, j = t // depth, lax.rem(t, depth)
        return j, kind // 2, (kind + 1) // 2

    top[...] = jnp.full_like(top, NEGATIVE)
    total[...] = jnp.zeros_like(total)
    acc[...] = jnp.zeros_like(acc)
    dq_acc[...] = jnp.zeros_like(dq_acc)

    def score_pass(t, carry):
        j, key_high, query_high = tile(t)
        score = lax.dot_general(
            k_sort[key_high, j],
            q_sort[query_high],
            (((1,), (1,)), ((), ())),
            preferred_element_type=jnp.float32,
        )
        query_blocks = [block_of(4 * z + 2 * side + c, query_high) for side in range(2)]
        best = top[query_high]
        for device in range(4):
            owner, side = device // 2, device % 2
            key_block = block_of(4 * j + 2 * side + owner, key_high)
            base, slope = [], []
            for query_block in query_blocks:
                live = (mask_ref[query_block, key_block] == 1) & (key_block <= query_block)
                same = live & (key_block == query_block)
                slope.append(same.astype(jnp.int32))
                base.append(jnp.where(same, 0, jnp.where(live, half, -1)))
            limit = jnp.where(in_first, base[0], base[1]) + query_row * jnp.where(
                in_first, slope[0], slope[1]
            )
            slab = score[device * half : (device + 1) * half]
            slab = jnp.where(key_row <= limit, slab, NEGATIVE)
            scores[t, device * half : (device + 1) * half] = slab
            best = jnp.maximum(best, jnp.max(slab.reshape(half // 8, 8, lanes), axis=0))
        top[query_high] = best
        return carry

    lax.fori_loop(0, tiles, score_pass, 0)
    v_relay()
    for high in range(2):
        best = jnp.max(top[high], axis=0, keepdims=True)
        top[high] = jnp.broadcast_to(best * factor, (8, lanes))

    def sum_pass(t, carry):
        j, key_high, query_high = tile(t)
        peak = top[query_high][0:1]
        spread_out = jnp.exp2(scores[t] * factor - peak)
        total[query_high] += jnp.sum(spread_out.reshape(4 * half // 8, 8, lanes), axis=0)
        return carry

    lax.fori_loop(0, tiles, sum_pass, 0)
    for high in range(2):
        whole = jnp.sum(total[high], axis=0, keepdims=True)
        shift = top[high][0:1] + jnp.log2(whole)
        top[high] = jnp.broadcast_to(shift, (8, lanes))

    def spread_rows(line):
        return jnp.broadcast_to(line, (8, line.shape[1]))

    copies.wait(g_in.at[1 - y], over_y + 3, beside)
    copies.wait(d_in.at[1 - y], over_y + 4, beside)
    for side in range(2):
        arrange(g_in, g_sort, side)
        d_pad[...] = jnp.zeros_like(d_pad)
        d_pad[:, 0 : d_in.shape[2]] = d_in[side]
        flipped = jnp.transpose(d_pad[...])
        flip = turned(4 * z + 2 * side + c)
        for h in range(GROUP):
            line = jnp.where(y == 1, flipped[GROUP + h : GROUP + h + 1], flipped[h : h + 1])
            first, second = line[:, 0:half], line[:, half:rows]
            at = (side * GROUP + h) * half
            d_sort[0, :, at : at + half] = spread_rows(jnp.where(flip, second, first))
            d_sort[1, :, at : at + half] = spread_rows(jnp.where(flip, first, second))
    v_finish()
    sort_keys(v_all, v_sort)

    def grad_pass(t, carry):
        j, key_high, query_high = tile(t)
        prob = jnp.exp2(scores[t] * factor - top[query_high][0:1])
        grads = g_sort[query_high]
        prob_grad = lax.dot_general(
            v_sort[key_high, j], grads, (((1,), (1,)), ((), ())), preferred_element_type=jnp.float32
        )
        score_grad = (prob * (prob_grad - d_sort[query_high][0:1])).astype(jnp.bfloat16)
        acc[key_high, j, :, HD : 2 * HD] += jnp.dot(
            prob.astype(jnp.bfloat16), grads, preferred_element_type=jnp.float32
        )
        acc[key_high, j, :, 0:HD] += jnp.dot(
            score_grad, q_sort[query_high], preferred_element_type=jnp.float32
        )
        dq_acc[query_high] += lax.dot_general(
            k_sort[key_high, j],
            score_grad,
            (((0,), (0,)), ((), ())),
            preferred_element_type=jnp.float32,
        )
        return carry

    lax.fori_loop(0, tiles, grad_pass, 0)

    def finish_part(index, carry):
        j, device = index // 4, lax.rem(index, 4)
        owner, side = device // 2, lax.rem(device, 2)
        flip = turned(4 * j + 2 * side + owner)
        at = pl.ds(pl.multiple_of(device * half, half), half)
        low, high = acc[0, j, at], acc[1, j, at]
        scale = jnp.where(
            lax.broadcasted_iota(jnp.int32, (half, 2 * HD), 1) < HD, jnp.float32(scaling), 1.0
        )
        first = jnp.where(flip, high, low) * scale
        second = jnp.where(flip, low, high) * scale
        part[j, owner, side, 0:half] = first.astype(part.dtype)
        part[j, owner, side, half:rows] = second.astype(part.dtype)
        return carry

    lax.fori_loop(0, 4 * depth, finish_part, 0)
    by_core = copies.slots(depth)
    for k in list(range(1, depth)) + [0]:
        copies.send(part.at[far(k), 1 - c], core_in.at[far(k)], by_core + k, core)

    for high in range(2):
        q_turned = (jnp.transpose(dq_acc[high]) * scaling).astype(jnp.bfloat16)
        q_sort[high] = q_turned
    for side in range(2):
        flip = turned(4 * z + 2 * side + c)
        for h in range(GROUP):
            at = (side * GROUP + h) * half
            low, high = q_sort[0, at : at + half], q_sort[1, at : at + half]
            h_q[y, c, side, 0:half, h * HD : (h + 1) * HD] = jnp.where(flip, high, low)
            h_q[y, c, side, half:rows, h * HD : (h + 1) * HD] = jnp.where(flip, low, high)

    def wide(ref):
        return ref[...].astype(jnp.float32)

    by_plane = copies.slots(depth)
    for k in list(range(1, depth)) + [0]:
        j = far(k)
        copies.wait(core_in.at[j], by_core + k, core)
        added = wide(part.at[j, c]) + wide(core_in.at[j])
        if k == 0:
            summed = added
        else:
            sum_out[k] = added.astype(sum_out.dtype)
            copies.send(sum_out.at[k], z_in.at[k], by_plane + k, plane(j))

    def quad_start(ref):
        first = copies.slots(3)
        here = ref.at[y, c]
        copies.send(here, here, first, beside)
        copies.send(here, here, first + 1, core)

        def relay():
            there = ref.at[1 - y, c]
            copies.wait(there, first, beside)
            copies.send(there, there, first + 2, core)

        def finish():
            copies.wait(ref.at[y, 1 - c], first + 1, core)
            copies.wait(ref.at[1 - y, 1 - c], first + 2, core)

        return relay, finish

    q_relay, q_finish = quad_start(h_q)
    w_relay(1)
    q_relay()
    for k in range(1, depth):
        copies.wait(z_in.at[k], by_plane + k, core)
        summed = summed + wide(z_in.at[k])
    h_kv[y, c] = summed.astype(h_kv.dtype)
    kv_relay, kv_finish = quad_start(h_kv)
    for step in range(2, depth - 1):
        w_relay(step)
    kv_relay()
    q_finish()
    kv_finish()

    heads = jnp.concatenate(
        [h_q[g].reshape(4 * rows, WIDE) for g in range(KVH)]
        + [
            h_kv[g, :, :, :, part_of * HD : (part_of + 1) * HD].reshape(4 * rows, HD)
            for part_of in range(2)
            for g in range(KVH)
        ],
        axis=1,
    )
    step_of = jnp.where(2 * z >= depth, depth - 1, 1)
    mine = 2 * y + c
    y_recv = [copies.slots(4 * depth) for _ in range(1)][0]
    for k in range(depth):
        if k == depth - 1:
            w_relay(depth - 1)
        j = lax.rem(z + k * step_of, depth)
        if k > 0:
            w_finish(j, None)
        block = lax.dot_general(
            heads, w_all[j], (((1,), (1,)), ((), ())), preferred_element_type=jnp.float32
        )
        y_out[j] = block.astype(y_out.dtype).reshape(2, 2, rows, shard)
        for device, owner, side in (
            (beside, c, 1 - y),
            (corner, 1 - c, 1 - y),
            (core, 1 - c, y),
        ):
            copies.send(
                y_out.at[j, owner, side], y_in.at[j, mine], y_recv + 4 * j + mine, device
            )
    for k in range(depth):
        j = lax.rem(z + k * step_of, depth)
        for source, device in (
            (2 * y + 1 - c, core),
            (2 * (1 - y) + c, beside),
            (2 * (1 - y) + 1 - c, corner),
        ):
            copies.wait(y_in.at[j, source], y_recv + 4 * j + source, device)
        y_in[j, mine] = y_out[j, c, y]
    for j in range(depth):
        for source in range(4):
            at = (4 * j + source) * shard
            out_ref[:, at : at + shard] = y_in[j, source]
    copies.drain()


def layer_grads(order, mask, queries, out_grad, row_delta, keys, values, weight, count):
    depth = count // 4
    rows = queries.shape[0]
    half = rows // 2
    lanes = 2 * GROUP * half
    shard, qkv = weight.shape
    low, wide = jnp.bfloat16, jnp.float32
    smem = pl.BlockSpec(memory_space=pltpu.SMEM)
    vmem = pl.BlockSpec(memory_space=pltpu.VMEM)
    anywhere = pl.BlockSpec(memory_space=pl.ANY)
    kv_shape = (depth, 2, 2, rows, HD)
    pair = (2, rows, 2 * HD)
    return pl.pallas_call(
        functools.partial(layer_kernel, depth),
        out_shape=jax.ShapeDtypeStruct((rows, count * shard), low),
        in_specs=[smem, smem] + [anywhere] * 6,
        out_specs=vmem,
        scratch_shapes=[
            pltpu.VMEM(kv_shape, low),
            pltpu.VMEM(kv_shape, low),
            pltpu.VMEM((2, rows, WIDE), low),
            pltpu.VMEM((2, rows, WIDE), low),
            pltpu.VMEM((2,) + row_delta.shape, wide),
            pltpu.VMEM((depth, shard, qkv), low),
            pltpu.VMEM((2, depth, 4 * half, HD), low),
            pltpu.VMEM((2, depth, 4 * half, HD), low),
            pltpu.VMEM((2, lanes, HD), low),
            pltpu.VMEM((2, lanes, HD), low),
            pltpu.VMEM((2, 8, lanes), wide),
            pltpu.VMEM((rows, 128), wide),
            pltpu.VMEM((3 * depth, 4 * half, lanes), wide),
            pltpu.VMEM((2, 8, lanes), wide),
            pltpu.VMEM((2, 8, lanes), wide),
            pltpu.VMEM((2, HD, lanes), wide),
            pltpu.VMEM((2, depth, 4 * half, 2 * HD), wide),
            pltpu.VMEM((depth, 2) + pair, low),
            pltpu.VMEM((depth,) + pair, low),
            pltpu.VMEM((depth,) + pair, low),
            pltpu.VMEM((depth,) + pair, low),
            pltpu.VMEM((2, 2, 2, rows, WIDE), low),
            pltpu.VMEM((2, 2, 2, rows, 2 * HD), low),
            pltpu.VMEM((depth, 2, 2, rows, shard), low),
            pltpu.VMEM((depth, 4, rows, shard), low),
            pltpu.SemaphoreType.DMA((6,)),
            pltpu.SemaphoreType.DMA((64 + 64 * depth,)),
            pltpu.SemaphoreType.DMA((64 + 32 * depth,)),
        ],
        compiler_params=pltpu.CompilerParams(
            collective_id=0, has_side_effects=True, vmem_limit_bytes=67043328
        ),
        name="layer_grads",
    )(order, mask, queries, out_grad, row_delta, keys, values, weight)


def swapped(array, axis, apart):
    return lax.ppermute(array, axis, [(i, i ^ 1 << apart) for i in range(lax.axis_size(axis))])


def body(
    queries,
    keys,
    values,
    out_grad,
    row_delta,
    layer_input,
    norm_gain,
    qkv_weight,
    block_order,
    block_mask,
    frame_owner,
    vision_features,
    post_gain,
    projector,
):
    tok_rows = queries.shape[0]
    half_len = tok_rows // 2
    my_index = lax.axis_index("seq")
    my_blocks = lax.dynamic_slice_in_dim(block_order, 2 * my_index, 2, 0)
    count = lax.axis_size("seq")
    norm_grad = layer_grads(
        block_order, block_mask, queries, out_grad, row_delta, keys, values, qkv_weight, count
    )
    inputs = layer_input.astype(jnp.float32)
    inverse = lax.rsqrt(jnp.mean(inputs * inputs, axis=1, keepdims=True) + EPSILON)
    scaled = norm_grad.astype(jnp.float32) * norm_gain
    token_grad = (
        inverse * scaled - inputs * inverse**3 * jnp.mean(scaled * inputs, axis=1, keepdims=True)
    ).astype(jnp.bfloat16)
    frame_table = jnp.arange(frame_owner.shape[0], dtype=jnp.int32)
    my_frame = jnp.sum(jnp.where(frame_owner == my_index, frame_table, 0))
    keep_first = my_blocks[0] // 2 == my_frame
    kept_block = jnp.where(keep_first, my_blocks[0], my_blocks[1])
    leading = kept_block % 2 == 0
    halves = token_grad.reshape(2, half_len, token_grad.shape[1])
    kept = jnp.where(keep_first, halves[0], halves[1])
    sending = jnp.where(keep_first, halves[1], halves[0])
    received = swapped(sending, "seq", 0)
    frame_rows = jnp.where(
        leading,
        jnp.concatenate([kept, received], axis=0),
        jnp.concatenate([received, kept], axis=0),
    )
    post_grad = jnp.dot(frame_rows, projector.T, preferred_element_type=jnp.float32)
    features = vision_features[0].astype(jnp.float32)
    centered = features - jnp.mean(features, axis=1, keepdims=True)
    deviation = lax.rsqrt(jnp.mean(centered * centered, axis=1, keepdims=True) + EPSILON)
    normed = centered * deviation
    weighted = post_grad * post_gain
    encoder_grad = (
        deviation
        * (
            weighted
            - jnp.mean(weighted, axis=1, keepdims=True)
            - normed * jnp.mean(weighted * normed, axis=1, keepdims=True)
        )
    ).astype(jnp.bfloat16)
    return (token_grad, encoder_grad[None])


def solution(mesh):
    placed = (
        P(("batch", "seq"), None),
        P(("batch", "seq"), None),
        P(("batch", "seq"), None),
        P(("batch", "seq"), None),
        P(("batch", "seq"), None),
        P(("batch", "seq"), None),
        P(),
        P("seq", None),
        P("batch"),
        P("batch", None),
        P("batch"),
        P(("batch", "seq"), None, None),
        P(),
        P(),
    )
    return jax.shard_map(
        body,
        mesh=mesh,
        in_specs=placed,
        out_specs=(P(("batch", "seq"), None), P(("batch", "seq"), None, None)),
        check_vma=False,
    )
```

```python
import functools

import jax
import jax.numpy as jnp
from jax import lax
from jax.experimental import pallas as pl
from jax.experimental.pallas import tpu as pltpu
from jax.sharding import PartitionSpec as P

HQ = 14
KVH = 2
HD = 128
GROUP = HQ // KVH
WIDE = GROUP * HD
LOG2E = 1.4426950408889634
EPSILON = 1e-06
NEGATIVE = -1e30
PIECES = 4
MESH = pl.DeviceIdType.MESH


def when(condition, action):
    if condition is None:
        action()
    else:
        pl.when(condition)(action)


def split_rows(size, count):
    tiles = size // 16
    edges = [tiles * i // count for i in range(count + 1)]
    return [(16 * a, 16 * (b - a)) for a, b in zip(edges, edges[1:]) if b > a]


class Copies:
    def __init__(self, send_sem, recv_sem):
        self.send_sem, self.recv_sem = send_sem, recv_sem
        self.sends, self.recvs = 0, 0
        self.started = []

    def slots(self, count=1):
        self.recvs += count
        return self.recvs - count

    def send(self, src, dst, recv, device, condition=None):
        copy = pltpu.make_async_remote_copy(
            src_ref=src,
            dst_ref=dst,
            send_sem=self.send_sem.at[self.sends],
            recv_sem=self.recv_sem.at[recv],
            device_id=device,
            device_id_type=MESH,
        )
        self.sends += 1
        when(condition, copy.start)
        self.started.append((condition, copy))

    def wait(self, ref, recv, device, condition=None):
        copy = pltpu.make_async_remote_copy(
            src_ref=ref,
            dst_ref=ref,
            send_sem=self.send_sem.at[0],
            recv_sem=self.recv_sem.at[recv],
            device_id=device,
            device_id_type=MESH,
        )
        when(condition, copy.wait_recv)

    def drain(self):
        for condition, copy in self.started:
            when(condition, copy.wait_send)


def layer_kernel(
    depth,
    counts,
    order_ref,
    mask_ref,
    queries_ref,
    grads_ref,
    delta_hbm,
    keys_ref,
    values_ref,
    weight_ref,
    out_ref,
    kv_swap,
    k_all,
    v_all,
    q_in,
    g_in,
    d_in,
    w_all,
    k_sort,
    v_sort,
    q_sort,
    g_sort,
    d_sort,
    scores,
    top,
    total,
    dq_acc,
    acc,
    part,
    core_in,
    sum_out,
    z_in,
    h_q,
    h_kv,
    y_out,
    y_in,
    load_sem,
    send_sem,
    recv_sem,
):
    me = lax.axis_index("seq")
    batch = lax.axis_index("batch")
    x = lax.rem(batch, 2)
    z, y, c = me // 4, lax.rem(me // 2, 2), lax.rem(me, 2)
    rows = q_in.shape[1]
    half = rows // 2
    lanes = 2 * GROUP * half
    shard = weight_ref.shape[0]
    scaling = HD ** (-0.5)
    factor = scaling * LOG2E

    up, down = {"seq": me + 4}, {"seq": me - 4}
    beside, core = {"seq": me + 2 - 4 * y}, {"seq": me + 1 - 2 * c}
    corner = {"seq": me + 2 - 4 * y + 1 - 2 * c}
    across = {"batch": batch + 1 - 2 * x}
    has_up, has_down = z < depth - 1, z > 0

    def far(k):
        return lax.rem(z + k, depth)

    def behind(k):
        return lax.rem(z + depth - k, depth)

    def plane(j):
        return {"seq": 4 * j + 2 * y + c}

    def head_at(ref, side, width):
        return ref.at[:, pl.ds(pl.multiple_of(side * width, 128), width)]

    def load(src, dst, index):
        copy = pltpu.make_async_copy(src, dst, load_sem.at[index])
        copy.start()
        return copy

    load_swap = [
        load(head_at(ref, 1 - y, HD), kv_swap.at[i], 6 + i)
        for i, ref in enumerate((keys_ref, values_ref))
    ]
    load_k = load(head_at(keys_ref, y, HD), k_all.at[z, c, y], 0)
    load_v = load(head_at(values_ref, y, HD), v_all.at[z, c, y], 1)
    load_w = load(weight_ref, w_all.at[z], 2)
    load_q = load(head_at(queries_ref, y, WIDE), q_in.at[y], 3)
    load_g = load(head_at(grads_ref, y, WIDE), g_in.at[y], 4)
    load_d = load(delta_hbm, d_in.at[y], 5)

    barrier = pltpu.get_barrier_semaphore()
    peers = [beside, core, corner, across] + [plane(far(k)) for k in range(1, depth)]
    for peer in peers:
        pl.semaphore_signal(barrier, inc=1, device_id=peer, device_id_type=MESH)
    pl.semaphore_wait(barrier, len(peers))

    copies = Copies(send_sem, recv_sem)

    over_y = copies.slots(5)
    for i, ref in enumerate((k_all, v_all)):
        load_swap[i].wait()
        copies.send(kv_swap.at[i], ref.at[z, c, y], over_y + i, beside)
    copies.send(head_at(queries_ref, 1 - y, WIDE), q_in.at[y], over_y + 2, beside)
    copies.send(head_at(grads_ref, 1 - y, WIDE), g_in.at[y], over_y + 3, beside)
    copies.send(delta_hbm, d_in.at[y], over_y + 4, beside)

    def spread(ref, load_own, swap):
        arrive = copies.slots(2 * depth)
        shared = copies.slots(2)

        def own(side, index):
            for k in range(depth - 1, 0, -1):
                copies.send(
                    ref.at[z, c, side], ref.at[z, c, side], arrive + 2 * k + index, plane(far(k))
                )
            copies.send(ref.at[z, c, side], ref.at[z, c, side], shared + index, core)

        def first():
            load_own.wait()
            own(y, 0)

        def second():
            copies.wait(ref.at[z, c, 1 - y], swap, beside)
            own(1 - y, 1)

        passed = copies.slots(depth)

        def relay():
            for k in range(1, depth):
                j = behind(k)
                for index in range(2):
                    side = y if index == 0 else 1 - y
                    copies.wait(ref.at[j, c, side], arrive + 2 * k + index, core)
                copies.send(ref.at[j, c], ref.at[j, c], passed + k, core)

        def finish():
            for index in range(2):
                side = y if index == 0 else 1 - y
                copies.wait(ref.at[z, 1 - c, side], shared + index, core)
            for k in range(1, depth):
                copies.wait(ref.at[behind(k), 1 - c], passed + k, core)

        return first, second, relay, finish

    k_first, k_second, k_relay, k_finish = spread(k_all, load_k, over_y)
    v_first, v_second, v_relay, v_finish = spread(v_all, load_v, over_y + 1)
    k_first()
    k_second()
    v_first()
    v_second()

    own_part = shard // 32 * 16
    between = shard - 2 * own_part
    pieces = split_rows(own_part, PIECES)

    def w_at(j, side, start, size):
        base = pl.multiple_of(side * (shard - own_part) + start, 16)
        return w_all.at[j, pl.ds(base, size)]

    def w_middle(j):
        return w_all.at[j, pl.ds(own_part, between)]

    count = len(pieces)
    w_recv = [copies.slots(depth) for _ in range(count + 1)]
    w_cross = [copies.slots(depth) for _ in range(count)]

    parts = list(range(count + (between > 0)))

    def w_send(j, upward, downward, some):
        for i in some:
            ref = w_at(j, x, *pieces[i]) if i < count else w_middle(j)
            if upward is not None:
                copies.send(ref, ref, w_recv[i] + j, up, upward)
            if downward is not None:
                copies.send(ref, ref, w_recv[i] + j, down, downward)

    def w_line(step, i):
        for j, present, upward in (
            (z - step, z - step >= 0, True),
            (z + step, z + step < depth, False),
        ):
            at = jnp.clip(j, 0, depth - 1)
            ref = w_at(at, x, *pieces[i]) if i < count else w_middle(at)
            yield at, present, upward, ref

    def w_take(step, i):
        for at, present, upward, ref in w_line(step, i):
            copies.wait(ref, w_recv[i] + at, core, present)
            if i < count:
                copies.send(ref, ref, w_cross[i] + at, across, present)

    def w_pass(step, i):
        if step == depth - 1:
            return
        for at, present, upward, ref in w_line(step, i):
            go = jnp.logical_and(present, has_up if upward else has_down)
            copies.send(ref, ref, w_recv[i] + at, up if upward else down, go)

    def w_relay(step, some):
        for i in some:
            w_take(step, i)
            w_pass(step, i)

    def w_finish(j, other):
        for i in range(count):
            copies.wait(w_at(j, 1 - x, *pieces[i]), w_cross[i] + j, across, other)

    load_w.wait()
    w_send(z, has_up, has_down, parts)

    def turned(device):
        return order_ref[2 * device] > order_ref[2 * device + 1]

    def arrange(source, target, side):
        flip = turned(4 * z + 2 * side + c)
        for h in range(GROUP):
            first = source[side, 0:half, h * HD : (h + 1) * HD]
            second = source[side, half:rows, h * HD : (h + 1) * HD]
            at = (side * GROUP + h) * half
            target[0, at : at + half] = jnp.where(flip, second, first)
            target[1, at : at + half] = jnp.where(flip, first, second)

    for copy in (load_q, load_g, load_d):
        copy.wait()
    k_relay()
    copies.wait(q_in.at[1 - y], over_y + 2, beside)
    for side in range(2):
        arrange(q_in, q_sort, side)

    def sort_keys(source, target):
        def one(index, carry):
            j, device = index // 4, lax.rem(index, 4)
            owner, side = device // 2, lax.rem(device, 2)
            flip = turned(4 * j + 2 * side + owner)
            first = source[j, owner, side, 0:half]
            second = source[j, owner, side, half:rows]
            at = pl.ds(pl.multiple_of(device * half, half), half)
            target[0, j, at] = jnp.where(flip, second, first)
            target[1, j, at] = jnp.where(flip, first, second)
            return carry

        lax.fori_loop(0, 4 * depth, one, 0)

    k_finish()
    sort_keys(k_all, k_sort)

    tiles = 3 * depth
    lane = lax.broadcasted_iota(jnp.int32, (1, lanes), 1)
    query_row = lax.rem(lane, half)
    in_first = lane < GROUP * half
    key_row = lax.broadcasted_iota(jnp.int32, (half, lanes), 0)

    def block_of(device, high):
        one, two = order_ref[2 * device], order_ref[2 * device + 1]
        return jnp.where(high == 1, jnp.maximum(one, two), jnp.minimum(one, two))

    def tile(t):
        kind, j = t // depth, lax.rem(t, depth)
        return j, kind // 2, (kind + 1) // 2

    top[...] = jnp.full_like(top, NEGATIVE)
    total[...] = jnp.zeros_like(total)
    acc[...] = jnp.zeros_like(acc)
    dq_acc[...] = jnp.zeros_like(dq_acc)

    def score_pass(t, carry):
        j, key_high, query_high = tile(t)
        score = lax.dot_general(
            k_sort[key_high, j],
            q_sort[query_high],
            (((1,), (1,)), ((), ())),
            preferred_element_type=jnp.float32,
        )
        query_blocks = [block_of(4 * z + 2 * side + c, query_high) for side in range(2)]
        best = top[query_high]
        for device in range(4):
            owner, side = device // 2, device % 2
            key_block = block_of(4 * j + 2 * side + owner, key_high)
            base, slope = [], []
            for query_block in query_blocks:
                live = (mask_ref[query_block, key_block] == 1) & (key_block <= query_block)
                same = live & (key_block == query_block)
                slope.append(same.astype(jnp.int32))
                base.append(jnp.where(same, 0, jnp.where(live, half, -1)))
            limit = jnp.where(in_first, base[0], base[1]) + query_row * jnp.where(
                in_first, slope[0], slope[1]
            )
            slab = score[device * half : (device + 1) * half]
            slab = jnp.where(key_row <= limit, slab, NEGATIVE)
            scores[t, device * half : (device + 1) * half] = slab
            best = jnp.maximum(best, jnp.max(slab.reshape(half // 8, 8, lanes), axis=0))
        top[query_high] = best
        return carry

    lax.fori_loop(0, tiles, score_pass, 0)
    v_relay()
    for high in range(2):
        best = jnp.max(top[high], axis=0, keepdims=True)
        top[high] = jnp.broadcast_to(best * factor, (8, lanes))

    def sum_pass(t, carry):
        j, key_high, query_high = tile(t)
        peak = top[query_high][0:1]
        spread_out = jnp.exp2(scores[t] * factor - peak)
        total[query_high] += jnp.sum(spread_out.reshape(4 * half // 8, 8, lanes), axis=0)
        return carry

    lax.fori_loop(0, tiles, sum_pass, 0)
    for high in range(2):
        whole = jnp.sum(total[high], axis=0, keepdims=True)
        shift = top[high][0:1] + jnp.log2(whole)
        top[high] = jnp.broadcast_to(shift, (8, lanes))

    def spread_rows(line):
        return jnp.broadcast_to(line, (8, line.shape[1]))

    copies.wait(g_in.at[1 - y], over_y + 3, beside)
    copies.wait(d_in.at[1 - y], over_y + 4, beside)
    for side in range(2):
        arrange(g_in, g_sort, side)
        flip = turned(4 * z + 2 * side + c)
        for h in range(GROUP):
            line = jnp.where(y == 1, d_in[side, GROUP + h : GROUP + h + 1], d_in[side, h : h + 1])
            first, second = line[:, 0:half], line[:, half:rows]
            at = (side * GROUP + h) * half
            d_sort[0, :, at : at + half] = spread_rows(jnp.where(flip, second, first))
            d_sort[1, :, at : at + half] = spread_rows(jnp.where(flip, first, second))
    v_finish()
    sort_keys(v_all, v_sort)

    def grad_pass(t, carry):
        j, key_high, query_high = tile(t)
        prob = jnp.exp2(scores[t] * factor - top[query_high][0:1])
        grads = g_sort[query_high]
        prob_grad = lax.dot_general(
            v_sort[key_high, j], grads, (((1,), (1,)), ((), ())), preferred_element_type=jnp.float32
        )
        score_grad = (prob * (prob_grad - d_sort[query_high][0:1])).astype(jnp.bfloat16)
        acc[key_high, j, :, HD : 2 * HD] += jnp.dot(
            prob.astype(jnp.bfloat16), grads, preferred_element_type=jnp.float32
        )
        acc[key_high, j, :, 0:HD] += jnp.dot(
            score_grad, q_sort[query_high], preferred_element_type=jnp.float32
        )
        dq_acc[query_high] += lax.dot_general(
            k_sort[key_high, j],
            score_grad,
            (((0,), (0,)), ((), ())),
            preferred_element_type=jnp.float32,
        )
        return carry

    scale = jnp.where(
        lax.broadcasted_iota(jnp.int32, (half, 2 * HD), 1) < HD, jnp.float32(scaling), 1.0
    )

    def finish_part(j):
        for device in range(4):
            owner, side = device // 2, device % 2
            flip = turned(4 * j + 2 * side + owner)
            at = slice(device * half, (device + 1) * half)
            low, high = acc[0, j, at], acc[1, j, at]
            first = jnp.where(flip, high, low) * scale
            second = jnp.where(flip, low, high) * scale
            part[j, owner, side, 0:half] = first.astype(part.dtype)
            part[j, owner, side, half:rows] = second.astype(part.dtype)

    def wide(ref):
        return ref[...].astype(jnp.float32)

    by_core, by_plane = copies.slots(depth), copies.slots(depth)

    def add_cores(k):
        j = far(k)
        copies.wait(core_in.at[j], by_core + k, core)
        added = wide(part.at[j, c]) + wide(core_in.at[j])
        if k > 0:
            sum_out[k] = added.astype(sum_out.dtype)
            copies.send(sum_out.at[k], z_in.at[k], by_plane + k, plane(j))
        return added

    order = list(range(1, depth)) + [0]
    taken = 0
    for index, k in enumerate(order):
        j = far(k)
        lax.fori_loop(0, 3, lambda kind, carry: grad_pass(kind * depth + j, carry), 0)
        finish_part(j)
        copies.send(part.at[j, 1 - c], core_in.at[j], by_core + k, core)
        if index > 0:
            add_cores(order[index - 1])
        if index < len(parts) - 1:
            w_take(1, parts[index])
            taken = index + 1

    for high in range(2):
        q_turned = (jnp.transpose(dq_acc[high]) * scaling).astype(jnp.bfloat16)
        q_sort[high] = q_turned
    for side in range(2):
        flip = turned(4 * z + 2 * side + c)
        for h in range(GROUP):
            at = (side * GROUP + h) * half
            low, high = q_sort[0, at : at + half], q_sort[1, at : at + half]
            h_q[y, c, side, 0:half, h * HD : (h + 1) * HD] = jnp.where(flip, high, low)
            h_q[y, c, side, half:rows, h * HD : (h + 1) * HD] = jnp.where(flip, low, high)

    def quad_start(ref):
        first = copies.slots(3)
        here = ref.at[y, c]
        copies.send(here, here, first, beside)
        copies.send(here, here, first + 1, core)

        def relay():
            there = ref.at[1 - y, c]
            copies.wait(there, first, beside)
            copies.send(there, there, first + 2, core)

        def finish():
            copies.wait(ref.at[y, 1 - c], first + 1, core)
            copies.wait(ref.at[1 - y, 1 - c], first + 2, core)

        return relay, finish

    q_relay, q_finish = quad_start(h_q)
    summed = add_cores(0)
    for i in parts[taken:]:
        w_take(1, i)
    for i in parts:
        w_pass(1, i)

    for k in range(1, depth):
        copies.wait(z_in.at[k], by_plane + k, core)
        summed = summed + wide(z_in.at[k])
    h_kv[y, c] = summed.astype(h_kv.dtype)
    kv_relay, kv_finish = quad_start(h_kv)
    near = list(range(2, depth - 1))
    for step in near[:-1]:
        w_relay(step, parts)
    cuts = [len(parts) * i // 4 for i in range(5)]
    groups = [parts[a:b] for a, b in zip(cuts, cuts[1:])]

    def w_some(index):
        if near:
            w_relay(near[-1], groups[index])

    w_some(0)
    q_relay()
    w_some(1)
    w_some(2)
    kv_relay()
    q_finish()
    kv_finish()

    heads = jnp.concatenate(
        [h_q[g].reshape(4 * rows, WIDE) for g in range(KVH)]
        + [
            h_kv[g, :, :, :, part_of * HD : (part_of + 1) * HD].reshape(4 * rows, HD)
            for part_of in range(2)
            for g in range(KVH)
        ],
        axis=1,
    )
    step_of = jnp.where(2 * z >= depth, depth - 1, 1)
    mine = 2 * y + c
    y_recv = copies.slots(4 * depth)

    def multiply(k):
        j = lax.rem(z + k * step_of, depth)
        if k > 0:
            w_finish(j, None)
        block = lax.dot_general(
            heads, w_all[j], (((1,), (1,)), ((), ())), preferred_element_type=jnp.float32
        )
        y_out[j] = block.astype(y_out.dtype).reshape(2, 2, rows, shard)
        for device, owner, side in (
            (beside, c, 1 - y),
            (corner, 1 - c, 1 - y),
            (core, 1 - c, y),
        ):
            copies.send(
                y_out.at[j, owner, side], y_in.at[j, mine], y_recv + 4 * j + mine, device
            )

    def collect(k):
        j = lax.rem(z + k * step_of, depth)
        for source, device in (
            (2 * y + 1 - c, core),
            (2 * (1 - y) + c, beside),
            (2 * (1 - y) + 1 - c, corner),
        ):
            copies.wait(y_in.at[j, source], y_recv + 4 * j + source, device)
        y_in[j, mine] = y_out[j, c, y]

    for k in range(depth - 1):
        if k == depth - 2:
            w_relay(depth - 1, groups[0])
            w_relay(depth - 1, groups[1])
        multiply(k)
        if k == 0:
            w_some(3)
    w_relay(depth - 1, groups[2])
    collect(0)
    w_relay(depth - 1, groups[3])
    for k in range(1, depth - 1):
        collect(k)
    multiply(depth - 1)
    collect(depth - 1)

    for j in range(depth):
        for source in range(4):
            at = (4 * j + source) * shard
            out_ref[:, at : at + shard] = y_in[j, source]
    copies.drain()
    counts.append((copies.sends, copies.recvs))


def layer_grads(arguments, count):
    order, mask, queries, out_grad, row_delta, keys, values, weight = arguments
    depth = count // 4
    rows = queries.shape[0]
    half = rows // 2
    lanes = 2 * GROUP * half
    shard, qkv = weight.shape
    low, wide = jnp.bfloat16, jnp.float32
    smem = pl.BlockSpec(memory_space=pltpu.SMEM)
    vmem = pl.BlockSpec(memory_space=pltpu.VMEM)
    anywhere = pl.BlockSpec(memory_space=pl.ANY)
    kv_shape = (depth, 2, 2, rows, HD)
    pair = (2, rows, 2 * HD)
    def build(counts, sends, recvs):
        return pl.pallas_call(
        functools.partial(layer_kernel, depth, counts),
        out_shape=jax.ShapeDtypeStruct((rows, count * shard), low),
        in_specs=[smem, smem] + [anywhere] * 6,
        out_specs=vmem,
        scratch_shapes=[
            pltpu.VMEM((2, rows, HD), low),
            pltpu.VMEM(kv_shape, low),
            pltpu.VMEM(kv_shape, low),
            pltpu.VMEM((2, rows, WIDE), low),
            pltpu.VMEM((2, rows, WIDE), low),
            pltpu.VMEM((2,) + row_delta.shape, wide),
            pltpu.VMEM((depth, shard, qkv), low),
            pltpu.VMEM((2, depth, 4 * half, HD), low),
            pltpu.VMEM((2, depth, 4 * half, HD), low),
            pltpu.VMEM((2, lanes, HD), low),
            pltpu.VMEM((2, lanes, HD), low),
            pltpu.VMEM((2, 8, lanes), wide),
            pltpu.VMEM((3 * depth, 4 * half, lanes), wide),
            pltpu.VMEM((2, 8, lanes), wide),
            pltpu.VMEM((2, 8, lanes), wide),
            pltpu.VMEM((2, HD, lanes), wide),
            pltpu.VMEM((2, depth, 4 * half, 2 * HD), wide),
            pltpu.VMEM((depth, 2) + pair, low),
            pltpu.VMEM((depth,) + pair, low),
            pltpu.VMEM((depth,) + pair, low),
            pltpu.VMEM((depth,) + pair, low),
            pltpu.VMEM((2, 2, 2, rows, WIDE), low),
            pltpu.VMEM((2, 2, 2, rows, 2 * HD), low),
            pltpu.VMEM((depth, 2, 2, rows, shard), low),
            pltpu.VMEM((depth, 4, rows, shard), low),
            pltpu.SemaphoreType.DMA((13,)),
            pltpu.SemaphoreType.DMA((sends,)),
            pltpu.SemaphoreType.DMA((recvs,)),
        ],
        compiler_params=pltpu.CompilerParams(
            collective_id=0, has_side_effects=True, vmem_limit_bytes=67043328
        ),
        name="layer_grads",
    )

    counts = []
    jax.eval_shape(build(counts, 4096, 4096), *arguments)
    return build([], *counts[0])(*arguments)


def swapped(array, axis, apart):
    return lax.ppermute(array, axis, [(i, i ^ 1 << apart) for i in range(lax.axis_size(axis))])


def body(
    queries,
    keys,
    values,
    out_grad,
    row_delta,
    layer_input,
    norm_gain,
    qkv_weight,
    block_order,
    block_mask,
    frame_owner,
    vision_features,
    post_gain,
    projector,
):
    arguments = (
        block_order,
        block_mask,
        queries,
        out_grad,
        row_delta.T,
        keys,
        values,
        qkv_weight,
    )
    tok_rows = queries.shape[0]
    half_len = tok_rows // 2
    my_index = lax.axis_index("seq")
    my_blocks = lax.dynamic_slice_in_dim(block_order, 2 * my_index, 2, 0)
    norm_grad = layer_grads(arguments, lax.axis_size("seq"))
    inputs = layer_input.astype(jnp.float32)
    inverse = lax.rsqrt(jnp.mean(inputs * inputs, axis=1, keepdims=True) + EPSILON)
    scaled = norm_grad.astype(jnp.float32) * norm_gain
    token_grad = (
        inverse * scaled - inputs * inverse**3 * jnp.mean(scaled * inputs, axis=1, keepdims=True)
    ).astype(jnp.bfloat16)
    frame_table = jnp.arange(frame_owner.shape[0], dtype=jnp.int32)
    my_frame = jnp.sum(jnp.where(frame_owner == my_index, frame_table, 0))
    keep_first = my_blocks[0] // 2 == my_frame
    kept_block = jnp.where(keep_first, my_blocks[0], my_blocks[1])
    leading = kept_block % 2 == 0
    halves = token_grad.reshape(2, half_len, token_grad.shape[1])
    kept = jnp.where(keep_first, halves[0], halves[1])
    sending = jnp.where(keep_first, halves[1], halves[0])
    received = swapped(sending, "seq", 0)
    frame_rows = jnp.where(
        leading,
        jnp.concatenate([kept, received], axis=0),
        jnp.concatenate([received, kept], axis=0),
    )
    post_grad = jnp.dot(frame_rows, projector.T, preferred_element_type=jnp.float32)
    features = vision_features[0].astype(jnp.float32)
    centered = features - jnp.mean(features, axis=1, keepdims=True)
    deviation = lax.rsqrt(jnp.mean(centered * centered, axis=1, keepdims=True) + EPSILON)
    normed = centered * deviation
    weighted = post_grad * post_gain
    encoder_grad = (
        deviation
        * (
            weighted
            - jnp.mean(weighted, axis=1, keepdims=True)
            - normed * jnp.mean(weighted * normed, axis=1, keepdims=True)
        )
    ).astype(jnp.bfloat16)
    return (token_grad, encoder_grad[None])


def solution(mesh):
    placed = (
        P(("batch", "seq"), None),
        P(("batch", "seq"), None),
        P(("batch", "seq"), None),
        P(("batch", "seq"), None),
        P(("batch", "seq"), None),
        P(("batch", "seq"), None),
        P(),
        P("seq", None),
        P("batch"),
        P("batch", None),
        P("batch"),
        P(("batch", "seq"), None, None),
        P(),
        P(),
    )
    return jax.shard_map(
        body,
        mesh=mesh,
        in_specs=placed,
        out_specs=(P(("batch", "seq"), None), P(("batch", "seq"), None, None)),
        check_vma=False,
    )
```

```python
import functools

import jax
import jax.numpy as jnp
from jax import lax
from jax.experimental import pallas as pl
from jax.experimental.pallas import tpu as pltpu
from jax.sharding import PartitionSpec as P

HQ = 14
KVH = 2
HD = 128
GROUP = HQ // KVH
WIDE = GROUP * HD
LOG2E = 1.4426950408889634
EPSILON = 1e-06
NEGATIVE = -1e30
PIECES = 4
MESH = pl.DeviceIdType.MESH


def when(condition, action):
    if condition is None:
        action()
    else:
        pl.when(condition)(action)


def split_rows(size, count):
    tiles = size // 16
    edges = [tiles * i // count for i in range(count + 1)]
    return [(16 * a, 16 * (b - a)) for a, b in zip(edges, edges[1:]) if b > a]


class Copies:
    def __init__(self, send_sem, recv_sem):
        self.send_sem, self.recv_sem = send_sem, recv_sem
        self.sends, self.recvs = 0, 0
        self.started = []

    def slots(self, count=1):
        self.recvs += count
        return self.recvs - count

    def send(self, src, dst, recv, device, condition=None):
        copy = pltpu.make_async_remote_copy(
            src_ref=src,
            dst_ref=dst,
            send_sem=self.send_sem.at[self.sends],
            recv_sem=self.recv_sem.at[recv],
            device_id=device,
            device_id_type=MESH,
        )
        self.sends += 1
        when(condition, copy.start)
        self.started.append((condition, copy))

    def wait(self, ref, recv, device, condition=None):
        copy = pltpu.make_async_remote_copy(
            src_ref=ref,
            dst_ref=ref,
            send_sem=self.send_sem.at[0],
            recv_sem=self.recv_sem.at[recv],
            device_id=device,
            device_id_type=MESH,
        )
        when(condition, copy.wait_recv)

    def drain(self):
        for condition, copy in self.started:
            when(condition, copy.wait_send)


def layer_kernel(
    depth,
    counts,
    order_ref,
    mask_ref,
    queries_ref,
    grads_ref,
    delta_hbm,
    keys_ref,
    values_ref,
    weight_ref,
    input_ref,
    gain_ref,
    owner_ref,
    features_ref,
    post_ref,
    projector_ref,
    token_ref,
    encoder_ref,
    gain_in,
    post_in,
    kv_swap,
    k_all,
    v_all,
    q_in,
    g_in,
    d_in,
    w_all,
    k_sort,
    v_sort,
    q_sort,
    g_sort,
    d_sort,
    scores,
    top,
    total,
    dq_acc,
    acc,
    part,
    core_in,
    sum_out,
    z_in,
    h_q,
    h_kv,
    y_out,
    y_in,
    x_in,
    x_cut,
    gain_cut,
    inverse,
    norm_cut,
    token,
    sending,
    received,
    features,
    normed,
    deviation,
    project,
    encoder,
    load_sem,
    send_sem,
    recv_sem,
):
    me = lax.axis_index("seq")
    batch = lax.axis_index("batch")
    x = lax.rem(batch, 2)
    z, y, c = me // 4, lax.rem(me // 2, 2), lax.rem(me, 2)
    rows = q_in.shape[1]
    half = rows // 2
    lanes = 2 * GROUP * half
    shard = weight_ref.shape[0]
    scaling = HD ** (-0.5)
    factor = scaling * LOG2E

    up, down = {"seq": me + 4}, {"seq": me - 4}
    beside, core = {"seq": me + 2 - 4 * y}, {"seq": me + 1 - 2 * c}
    corner = {"seq": me + 2 - 4 * y + 1 - 2 * c}
    across = {"batch": batch + 1 - 2 * x}
    has_up, has_down = z < depth - 1, z > 0

    def far(k):
        return lax.rem(z + k, depth)

    def behind(k):
        return lax.rem(z + depth - k, depth)

    def plane(j):
        return {"seq": 4 * j + 2 * y + c}

    def head_at(ref, side, width):
        return ref.at[:, pl.ds(pl.multiple_of(side * width, 128), width)]

    def load(src, dst, index):
        copy = pltpu.make_async_copy(src, dst, load_sem.at[index])
        copy.start()
        return copy

    load_swap = [
        load(head_at(ref, 1 - y, HD), kv_swap.at[i], 6 + i)
        for i, ref in enumerate((keys_ref, values_ref))
    ]
    load_k = load(head_at(keys_ref, y, HD), k_all.at[z, c, y], 0)
    load_v = load(head_at(values_ref, y, HD), v_all.at[z, c, y], 1)
    load_w = load(weight_ref, w_all.at[z], 2)
    load_q = load(head_at(queries_ref, y, WIDE), q_in.at[y], 3)
    load_g = load(head_at(grads_ref, y, WIDE), g_in.at[y], 4)
    load_d = load(delta_hbm, d_in.at[y], 5)
    load_x = load(input_ref, x_in, 8)
    load_f = load(features_ref.at[0], features, 9)
    load_n = [load(gain_ref, gain_in, 13), load(post_ref, post_in, 14)]

    barrier = pltpu.get_barrier_semaphore()
    peers = [beside, core, corner, across] + [plane(far(k)) for k in range(1, depth)]
    for peer in peers:
        pl.semaphore_signal(barrier, inc=1, device_id=peer, device_id_type=MESH)
    pl.semaphore_wait(barrier, len(peers))

    copies = Copies(send_sem, recv_sem)

    over_y = copies.slots(5)
    for i, ref in enumerate((k_all, v_all)):
        load_swap[i].wait()
        copies.send(kv_swap.at[i], ref.at[z, c, y], over_y + i, beside)
    copies.send(head_at(queries_ref, 1 - y, WIDE), q_in.at[y], over_y + 2, beside)
    copies.send(head_at(grads_ref, 1 - y, WIDE), g_in.at[y], over_y + 3, beside)
    copies.send(delta_hbm, d_in.at[y], over_y + 4, beside)

    def spread(ref, load_own, swap):
        arrive = copies.slots(2 * depth)
        shared = copies.slots(2)

        def own(side, index):
            for k in range(depth - 1, 0, -1):
                copies.send(
                    ref.at[z, c, side], ref.at[z, c, side], arrive + 2 * k + index, plane(far(k))
                )
            copies.send(ref.at[z, c, side], ref.at[z, c, side], shared + index, core)

        def first():
            load_own.wait()
            own(y, 0)

        def second():
            copies.wait(ref.at[z, c, 1 - y], swap, beside)
            own(1 - y, 1)

        passed = copies.slots(depth)

        def relay():
            for k in range(1, depth):
                j = behind(k)
                for index in range(2):
                    side = y if index == 0 else 1 - y
                    copies.wait(ref.at[j, c, side], arrive + 2 * k + index, core)
                copies.send(ref.at[j, c], ref.at[j, c], passed + k, core)

        def finish():
            for index in range(2):
                side = y if index == 0 else 1 - y
                copies.wait(ref.at[z, 1 - c, side], shared + index, core)
            for k in range(1, depth):
                copies.wait(ref.at[behind(k), 1 - c], passed + k, core)

        return first, second, relay, finish

    k_first, k_second, k_relay, k_finish = spread(k_all, load_k, over_y)
    v_first, v_second, v_relay, v_finish = spread(v_all, load_v, over_y + 1)
    k_first()
    k_second()
    v_first()
    v_second()

    own_part = shard // 32 * 16
    between = shard - 2 * own_part
    pieces = split_rows(own_part, PIECES)

    def w_at(j, side, start, size):
        base = pl.multiple_of(side * (shard - own_part) + start, 16)
        return w_all.at[j, pl.ds(base, size)]

    def w_middle(j):
        return w_all.at[j, pl.ds(own_part, between)]

    count = len(pieces)
    w_recv = [copies.slots(depth) for _ in range(count + 1)]
    w_cross = [copies.slots(depth) for _ in range(count)]

    parts = list(range(count + (between > 0)))

    def w_send(j, upward, downward, some):
        for i in some:
            ref = w_at(j, x, *pieces[i]) if i < count else w_middle(j)
            if upward is not None:
                copies.send(ref, ref, w_recv[i] + j, up, upward)
            if downward is not None:
                copies.send(ref, ref, w_recv[i] + j, down, downward)

    def w_line(step, i):
        for j, present, upward in (
            (z - step, z - step >= 0, True),
            (z + step, z + step < depth, False),
        ):
            at = jnp.clip(j, 0, depth - 1)
            ref = w_at(at, x, *pieces[i]) if i < count else w_middle(at)
            yield at, present, upward, ref

    def w_take(step, i):
        for at, present, upward, ref in w_line(step, i):
            copies.wait(ref, w_recv[i] + at, core, present)
            if i < count:
                copies.send(ref, ref, w_cross[i] + at, across, present)

    def w_pass(step, i):
        if step == depth - 1:
            return
        for at, present, upward, ref in w_line(step, i):
            go = jnp.logical_and(present, has_up if upward else has_down)
            copies.send(ref, ref, w_recv[i] + at, up if upward else down, go)

    def w_relay(step, some):
        for i in some:
            w_take(step, i)
            w_pass(step, i)

    def w_finish(j, other):
        for i in range(count):
            copies.wait(w_at(j, 1 - x, *pieces[i]), w_cross[i] + j, across, other)

    load_w.wait()
    w_send(z, has_up, has_down, parts)

    def turned(device):
        return order_ref[2 * device] > order_ref[2 * device + 1]

    def arrange(source, target, side):
        flip = turned(4 * z + 2 * side + c)
        for h in range(GROUP):
            first = source[side, 0:half, h * HD : (h + 1) * HD]
            second = source[side, half:rows, h * HD : (h + 1) * HD]
            at = (side * GROUP + h) * half
            target[0, at : at + half] = jnp.where(flip, second, first)
            target[1, at : at + half] = jnp.where(flip, first, second)

    for copy in (load_q, load_g, load_d):
        copy.wait()
    k_relay()
    copies.wait(q_in.at[1 - y], over_y + 2, beside)
    for side in range(2):
        arrange(q_in, q_sort, side)

    def sort_keys(source, target):
        def one(index, carry):
            j, device = index // 4, lax.rem(index, 4)
            owner, side = device // 2, lax.rem(device, 2)
            flip = turned(4 * j + 2 * side + owner)
            first = source[j, owner, side, 0:half]
            second = source[j, owner, side, half:rows]
            at = pl.ds(pl.multiple_of(device * half, half), half)
            target[0, j, at] = jnp.where(flip, second, first)
            target[1, j, at] = jnp.where(flip, first, second)
            return carry

        lax.fori_loop(0, 4 * depth, one, 0)

    k_finish()
    sort_keys(k_all, k_sort)

    tiles = 3 * depth
    lane = lax.broadcasted_iota(jnp.int32, (1, lanes), 1)
    query_row = lax.rem(lane, half)
    in_first = lane < GROUP * half
    key_row = lax.broadcasted_iota(jnp.int32, (half, lanes), 0)

    def block_of(device, high):
        one, two = order_ref[2 * device], order_ref[2 * device + 1]
        return jnp.where(high == 1, jnp.maximum(one, two), jnp.minimum(one, two))

    def tile(t):
        kind, j = t // depth, lax.rem(t, depth)
        return j, kind // 2, (kind + 1) // 2

    top[...] = jnp.full_like(top, NEGATIVE)
    total[...] = jnp.zeros_like(total)
    acc[...] = jnp.zeros_like(acc)
    dq_acc[...] = jnp.zeros_like(dq_acc)

    def score_pass(t, carry):
        j, key_high, query_high = tile(t)
        score = lax.dot_general(
            k_sort[key_high, j],
            q_sort[query_high],
            (((1,), (1,)), ((), ())),
            preferred_element_type=jnp.float32,
        )
        query_blocks = [block_of(4 * z + 2 * side + c, query_high) for side in range(2)]
        best = top[query_high]
        for device in range(4):
            owner, side = device // 2, device % 2
            key_block = block_of(4 * j + 2 * side + owner, key_high)
            base, slope = [], []
            for query_block in query_blocks:
                live = (mask_ref[query_block, key_block] == 1) & (key_block <= query_block)
                same = live & (key_block == query_block)
                slope.append(same.astype(jnp.int32))
                base.append(jnp.where(same, 0, jnp.where(live, half, -1)))
            limit = jnp.where(in_first, base[0], base[1]) + query_row * jnp.where(
                in_first, slope[0], slope[1]
            )
            slab = score[device * half : (device + 1) * half]
            slab = jnp.where(key_row <= limit, slab, NEGATIVE)
            scores[t, device * half : (device + 1) * half] = slab
            best = jnp.maximum(best, jnp.max(slab.reshape(half // 8, 8, lanes), axis=0))
        top[query_high] = best
        return carry

    load_p = load(projector_ref, project, 12)
    lax.fori_loop(0, tiles, score_pass, 0)
    v_relay()
    for high in range(2):
        best = jnp.max(top[high], axis=0, keepdims=True)
        top[high] = jnp.broadcast_to(best * factor, (8, lanes))

    def sum_pass(t, carry):
        j, key_high, query_high = tile(t)
        peak = top[query_high][0:1]
        spread_out = jnp.exp2(scores[t] * factor - peak)
        total[query_high] += jnp.sum(spread_out.reshape(4 * half // 8, 8, lanes), axis=0)
        return carry

    lax.fori_loop(0, tiles, sum_pass, 0)
    for high in range(2):
        whole = jnp.sum(total[high], axis=0, keepdims=True)
        shift = top[high][0:1] + jnp.log2(whole)
        top[high] = jnp.broadcast_to(shift, (8, lanes))

    def spread_rows(line):
        return jnp.broadcast_to(line, (8, line.shape[1]))

    copies.wait(g_in.at[1 - y], over_y + 3, beside)
    copies.wait(d_in.at[1 - y], over_y + 4, beside)
    for side in range(2):
        arrange(g_in, g_sort, side)
        flip = turned(4 * z + 2 * side + c)
        for h in range(GROUP):
            line = jnp.where(y == 1, d_in[side, GROUP + h : GROUP + h + 1], d_in[side, h : h + 1])
            first, second = line[:, 0:half], line[:, half:rows]
            at = (side * GROUP + h) * half
            d_sort[0, :, at : at + half] = spread_rows(jnp.where(flip, second, first))
            d_sort[1, :, at : at + half] = spread_rows(jnp.where(flip, first, second))
    v_finish()
    sort_keys(v_all, v_sort)

    def grad_pass(t, carry):
        j, key_high, query_high = tile(t)
        prob = jnp.exp2(scores[t] * factor - top[query_high][0:1])
        grads = g_sort[query_high]
        prob_grad = lax.dot_general(
            v_sort[key_high, j], grads, (((1,), (1,)), ((), ())), preferred_element_type=jnp.float32
        )
        score_grad = (prob * (prob_grad - d_sort[query_high][0:1])).astype(jnp.bfloat16)
        acc[key_high, j, :, HD : 2 * HD] += jnp.dot(
            prob.astype(jnp.bfloat16), grads, preferred_element_type=jnp.float32
        )
        acc[key_high, j, :, 0:HD] += jnp.dot(
            score_grad, q_sort[query_high], preferred_element_type=jnp.float32
        )
        dq_acc[query_high] += lax.dot_general(
            k_sort[key_high, j],
            score_grad,
            (((0,), (0,)), ((), ())),
            preferred_element_type=jnp.float32,
        )
        return carry

    scale = jnp.where(
        lax.broadcasted_iota(jnp.int32, (half, 2 * HD), 1) < HD, jnp.float32(scaling), 1.0
    )

    def finish_part(j):
        for device in range(4):
            owner, side = device // 2, device % 2
            flip = turned(4 * j + 2 * side + owner)
            at = slice(device * half, (device + 1) * half)
            low, high = acc[0, j, at], acc[1, j, at]
            first = jnp.where(flip, high, low) * scale
            second = jnp.where(flip, low, high) * scale
            part[j, owner, side, 0:half] = first.astype(part.dtype)
            part[j, owner, side, half:rows] = second.astype(part.dtype)

    def wide(ref):
        return ref[...].astype(jnp.float32)

    by_core, by_plane = copies.slots(depth), copies.slots(depth)

    def add_cores(k):
        j = far(k)
        copies.wait(core_in.at[j], by_core + k, core)
        added = wide(part.at[j, c]) + wide(core_in.at[j])
        if k > 0:
            sum_out[k] = added.astype(sum_out.dtype)
            copies.send(sum_out.at[k], z_in.at[k], by_plane + k, plane(j))
        return added

    order = list(range(1, depth)) + [0]
    taken = 0
    for index, k in enumerate(order):
        j = far(k)
        lax.fori_loop(0, 3, lambda kind, carry: grad_pass(kind * depth + j, carry), 0)
        finish_part(j)
        copies.send(part.at[j, 1 - c], core_in.at[j], by_core + k, core)
        if index > 0:
            add_cores(order[index - 1])
        if index < len(parts) - 1:
            w_take(1, parts[index])
            taken = index + 1

    for high in range(2):
        q_turned = (jnp.transpose(dq_acc[high]) * scaling).astype(jnp.bfloat16)
        q_sort[high] = q_turned
    for side in range(2):
        flip = turned(4 * z + 2 * side + c)
        for h in range(GROUP):
            at = (side * GROUP + h) * half
            low, high = q_sort[0, at : at + half], q_sort[1, at : at + half]
            h_q[y, c, side, 0:half, h * HD : (h + 1) * HD] = jnp.where(flip, high, low)
            h_q[y, c, side, half:rows, h * HD : (h + 1) * HD] = jnp.where(flip, low, high)

    def quad_start(ref):
        first = copies.slots(3)
        here = ref.at[y, c]
        copies.send(here, here, first, beside)
        copies.send(here, here, first + 1, core)

        def relay():
            there = ref.at[1 - y, c]
            copies.wait(there, first, beside)
            copies.send(there, there, first + 2, core)

        def finish():
            copies.wait(ref.at[y, 1 - c], first + 1, core)
            copies.wait(ref.at[1 - y, 1 - c], first + 2, core)

        return relay, finish

    q_relay, q_finish = quad_start(h_q)
    summed = add_cores(0)
    for i in parts[taken:]:
        w_take(1, i)
    for i in parts:
        w_pass(1, i)

    width = 4 * shard
    model = depth * width
    for copy in [load_x, load_f] + load_n:
        copy.wait()
    gain = gain_in[...].reshape(1, model)
    squares = jnp.zeros((rows, 1), jnp.float32)
    for j in range(depth):
        block = x_in[:, j * width : (j + 1) * width]
        x_cut[j] = block
        block = block.astype(jnp.float32)
        squares += jnp.sum(block * block, axis=1, keepdims=True)
        gain_cut[j] = jnp.broadcast_to(
            gain[:, j * width : (j + 1) * width], (8, width)
        )
    inverse[...] = jnp.broadcast_to(lax.rsqrt(squares / model + EPSILON), inverse.shape)
    seen = features[...].astype(jnp.float32)
    centered = seen - jnp.mean(seen, axis=1, keepdims=True)
    spread_of = lax.rsqrt(jnp.mean(centered * centered, axis=1, keepdims=True) + EPSILON)
    normed[...] = centered * spread_of
    deviation[...] = jnp.broadcast_to(spread_of, deviation.shape)

    for k in range(1, depth):
        copies.wait(z_in.at[k], by_plane + k, core)
        summed = summed + wide(z_in.at[k])
    h_kv[y, c] = summed.astype(h_kv.dtype)
    kv_relay, kv_finish = quad_start(h_kv)
    near = list(range(2, depth - 1))
    for step in near[:-1]:
        w_relay(step, parts)
    cuts = [len(parts) * i // 4 for i in range(5)]
    groups = [parts[a:b] for a, b in zip(cuts, cuts[1:])]

    def w_some(index):
        if near:
            w_relay(near[-1], groups[index])

    w_some(0)
    q_relay()
    w_some(1)
    w_some(2)
    kv_relay()
    q_finish()
    kv_finish()

    heads = jnp.concatenate(
        [h_q[g].reshape(4 * rows, WIDE) for g in range(KVH)]
        + [
            h_kv[g, :, :, :, part_of * HD : (part_of + 1) * HD].reshape(4 * rows, HD)
            for part_of in range(2)
            for g in range(KVH)
        ],
        axis=1,
    )
    step_of = jnp.where(2 * z >= depth, depth - 1, 1)
    mine = 2 * y + c
    y_recv = copies.slots(4 * depth)

    def multiply(k):
        j = lax.rem(z + k * step_of, depth)
        if k > 0:
            w_finish(j, None)
        block = lax.dot_general(
            heads, w_all[j], (((1,), (1,)), ((), ())), preferred_element_type=jnp.float32
        )
        y_out[j] = block.astype(y_out.dtype).reshape(2, 2, rows, shard)
        for device, owner, side in (
            (beside, c, 1 - y),
            (corner, 1 - c, 1 - y),
            (core, 1 - c, y),
        ):
            copies.send(
                y_out.at[j, owner, side], y_in.at[j, mine], y_recv + 4 * j + mine, device
            )

    def collect(k, dots):
        j = lax.rem(z + k * step_of, depth)
        for source, device in (
            (2 * y + 1 - c, core),
            (2 * (1 - y) + c, beside),
            (2 * (1 - y) + 1 - c, corner),
        ):
            copies.wait(y_in.at[j, source], y_recv + 4 * j + source, device)
        y_in[j, mine] = y_out[j, c, y]
        block = jnp.concatenate([wide(y_in.at[j, source]) for source in range(4)], axis=1)
        block = block * gain_cut[j][0:1]
        norm_cut[j] = block
        return dots + jnp.sum(block * x_cut[j].astype(jnp.float32), axis=1, keepdims=True)

    dots = jnp.zeros((rows, 1), jnp.float32)
    for k in range(depth - 1):
        if k == depth - 2:
            w_relay(depth - 1, groups[0])
            w_relay(depth - 1, groups[1])
        multiply(k)
        if k == 0:
            w_some(3)
    w_relay(depth - 1, groups[2])
    dots = collect(0, dots)
    w_relay(depth - 1, groups[3])
    for k in range(1, depth - 1):
        dots = collect(k, dots)
    multiply(depth - 1)
    dots = collect(depth - 1, dots)

    scale_in = inverse[:, 0:1]
    pull = scale_in * scale_in * scale_in * (dots / model)
    for j in range(depth):
        block = scale_in * norm_cut[j] - x_cut[j].astype(jnp.float32) * pull
        token[:, j * width : (j + 1) * width] = block.astype(token.dtype)

    start = jnp.int32(0)
    for frame in range(owner_ref.shape[0]):
        start = start + jnp.where(owner_ref[frame] == me, 2 * frame, 0)
    one, two = order_ref[2 * me], order_ref[2 * me + 1]
    keep_first = (one == start) | (one == start + 1)
    leading = jnp.where(keep_first, one, two) == start
    sending[...] = jnp.where(keep_first, token[half:rows], token[0:half])
    frame_recv = copies.slots(1)
    copies.send(sending, received, frame_recv, core)
    store_token = pltpu.make_async_copy(token, token_ref, load_sem.at[10])
    store_token.start()
    load_p.wait()
    kept = jnp.where(keep_first, token[0:half], token[half:rows])
    copies.wait(received, frame_recv, core)
    other = received[...]
    frame = jnp.concatenate(
        [jnp.where(leading, kept, other), jnp.where(leading, other, kept)], axis=0
    )
    post = lax.dot_general(
        frame, project[...], (((1,), (1,)), ((), ())), preferred_element_type=jnp.float32
    )
    post = post * post_in[...].reshape(1, post.shape[1])
    flat = normed[...]
    post = (
        post
        - jnp.mean(post, axis=1, keepdims=True)
        - flat * jnp.mean(post * flat, axis=1, keepdims=True)
    )
    encoder[...] = (deviation[:, 0:1] * post).astype(encoder.dtype)
    store_encoder = pltpu.make_async_copy(encoder, encoder_ref.at[0], load_sem.at[11])
    store_encoder.start()
    copies.drain()
    counts.append((copies.sends, copies.recvs))
    store_token.wait()
    store_encoder.wait()


def layer_grads(arguments, count):
    (
        order,
        mask,
        queries,
        out_grad,
        row_delta,
        keys,
        values,
        weight,
        layer_input,
        norm_gain,
        frame_owner,
        features,
        post_gain,
        projector,
    ) = arguments
    depth = count // 4
    rows = queries.shape[0]
    half = rows // 2
    lanes = 2 * GROUP * half
    shard, qkv = weight.shape
    low, wide = jnp.bfloat16, jnp.float32
    smem = pl.BlockSpec(memory_space=pltpu.SMEM)
    vmem = pl.BlockSpec(memory_space=pltpu.VMEM)
    anywhere = pl.BlockSpec(memory_space=pl.ANY)
    kv_shape = (depth, 2, 2, rows, HD)
    pair = (2, rows, 2 * HD)
    def build(counts, sends, recvs):
        return pl.pallas_call(
        functools.partial(layer_kernel, depth, counts),
        out_shape=(
            jax.ShapeDtypeStruct(layer_input.shape, low),
            jax.ShapeDtypeStruct(features.shape, low),
        ),
        in_specs=[smem, smem] + [anywhere] * 7 + [anywhere, smem, anywhere, anywhere, anywhere],
        out_specs=(anywhere, anywhere),
        scratch_shapes=[
            pltpu.VMEM(norm_gain.shape, wide),
            pltpu.VMEM(post_gain.shape, wide),
            pltpu.VMEM((2, rows, HD), low),
            pltpu.VMEM(kv_shape, low),
            pltpu.VMEM(kv_shape, low),
            pltpu.VMEM((2, rows, WIDE), low),
            pltpu.VMEM((2, rows, WIDE), low),
            pltpu.VMEM((2,) + row_delta.shape, wide),
            pltpu.VMEM((depth, shard, qkv), low),
            pltpu.VMEM((2, depth, 4 * half, HD), low),
            pltpu.VMEM((2, depth, 4 * half, HD), low),
            pltpu.VMEM((2, lanes, HD), low),
            pltpu.VMEM((2, lanes, HD), low),
            pltpu.VMEM((2, 8, lanes), wide),
            pltpu.VMEM((3 * depth, 4 * half, lanes), wide),
            pltpu.VMEM((2, 8, lanes), wide),
            pltpu.VMEM((2, 8, lanes), wide),
            pltpu.VMEM((2, HD, lanes), wide),
            pltpu.VMEM((2, depth, 4 * half, 2 * HD), wide),
            pltpu.VMEM((depth, 2) + pair, low),
            pltpu.VMEM((depth,) + pair, low),
            pltpu.VMEM((depth,) + pair, low),
            pltpu.VMEM((depth,) + pair, low),
            pltpu.VMEM((2, 2, 2, rows, WIDE), low),
            pltpu.VMEM((2, 2, 2, rows, 2 * HD), low),
            pltpu.VMEM((depth, 2, 2, rows, shard), low),
            pltpu.VMEM((depth, 4, rows, shard), low),
            pltpu.VMEM(layer_input.shape, low),
            pltpu.VMEM((depth, rows, 4 * shard), low),
            pltpu.VMEM((depth, 8, 4 * shard), wide),
            pltpu.VMEM((rows, 128), wide),
            pltpu.VMEM((depth, rows, 4 * shard), wide),
            pltpu.VMEM(layer_input.shape, low),
            pltpu.VMEM((half, layer_input.shape[1]), low),
            pltpu.VMEM((half, layer_input.shape[1]), low),
            pltpu.VMEM(features.shape[1:], low),
            pltpu.VMEM(features.shape[1:], wide),
            pltpu.VMEM((rows, 128), wide),
            pltpu.VMEM(projector.shape, low),
            pltpu.VMEM(features.shape[1:], low),
            pltpu.SemaphoreType.DMA((15,)),
            pltpu.SemaphoreType.DMA((sends,)),
            pltpu.SemaphoreType.DMA((recvs,)),
        ],
        compiler_params=pltpu.CompilerParams(
            collective_id=0, has_side_effects=True, vmem_limit_bytes=67043328
        ),
        name="layer_grads",
    )

    counts = []
    jax.eval_shape(build(counts, 4096, 4096), *arguments)
    return build([], *counts[0])(*arguments)


def body(
    queries,
    keys,
    values,
    out_grad,
    row_delta,
    layer_input,
    norm_gain,
    qkv_weight,
    block_order,
    block_mask,
    frame_owner,
    vision_features,
    post_gain,
    projector,
):
    arguments = (
        block_order,
        block_mask,
        queries,
        out_grad,
        row_delta.T,
        keys,
        values,
        qkv_weight,
        layer_input,
        norm_gain,
        frame_owner,
        vision_features,
        post_gain,
        projector,
    )
    return layer_grads(arguments, lax.axis_size("seq"))


def solution(mesh):
    placed = (
        P(("batch", "seq"), None),
        P(("batch", "seq"), None),
        P(("batch", "seq"), None),
        P(("batch", "seq"), None),
        P(("batch", "seq"), None),
        P(("batch", "seq"), None),
        P(),
        P("seq", None),
        P("batch"),
        P("batch", None),
        P("batch"),
        P(("batch", "seq"), None, None),
        P(),
        P(),
    )
    return jax.shard_map(
        body,
        mesh=mesh,
        in_specs=placed,
        out_specs=(P(("batch", "seq"), None), P(("batch", "seq"), None, None)),
        check_vma=False,
    )
```

```python
import functools

import jax
import jax.numpy as jnp
from jax import lax
from jax.experimental import pallas as pl
from jax.experimental.pallas import tpu as pltpu
from jax.sharding import PartitionSpec as P

HQ = 14
KVH = 2
HD = 128
GROUP = HQ // KVH
WIDE = GROUP * HD
LOG2E = 1.4426950408889634
EPSILON = 1e-06
NEGATIVE = -1e30
PIECES = 4
CUTS = 4
MESH = pl.DeviceIdType.MESH


def when(condition, action):
    if condition is None:
        action()
    else:
        pl.when(condition)(action)


def split_rows(size, count):
    tiles = size // 16
    edges = [tiles * i // count for i in range(count + 1)]
    return [(16 * a, 16 * (b - a)) for a, b in zip(edges, edges[1:]) if b > a]


class Copies:
    def __init__(self, send_sem, recv_sem):
        self.send_sem, self.recv_sem = send_sem, recv_sem
        self.sends, self.recvs = 0, 0
        self.started = []

    def slots(self, count=1):
        self.recvs += count
        return self.recvs - count

    def send(self, src, dst, recv, device, condition=None):
        copy = pltpu.make_async_remote_copy(
            src_ref=src,
            dst_ref=dst,
            send_sem=self.send_sem.at[self.sends],
            recv_sem=self.recv_sem.at[recv],
            device_id=device,
            device_id_type=MESH,
        )
        self.sends += 1
        when(condition, copy.start)
        self.started.append((condition, copy))

    def wait(self, ref, recv, device, condition=None):
        copy = pltpu.make_async_remote_copy(
            src_ref=ref,
            dst_ref=ref,
            send_sem=self.send_sem.at[0],
            recv_sem=self.recv_sem.at[recv],
            device_id=device,
            device_id_type=MESH,
        )
        when(condition, copy.wait_recv)

    def drain(self):
        for condition, copy in self.started:
            when(condition, copy.wait_send)


def layer_kernel(
    depth,
    counts,
    order_ref,
    mask_ref,
    queries_ref,
    grads_ref,
    delta_hbm,
    keys_ref,
    values_ref,
    weight_ref,
    input_ref,
    gain_ref,
    owner_ref,
    features_ref,
    post_ref,
    projector_ref,
    token_ref,
    encoder_ref,
    gain_in,
    post_in,
    kv_swap,
    k_all,
    v_all,
    q_in,
    g_in,
    d_in,
    w_all,
    k_sort,
    v_sort,
    q_sort,
    g_sort,
    d_sort,
    scores,
    top,
    total,
    dq_acc,
    acc,
    part,
    core_in,
    sum_out,
    z_in,
    h_q,
    h_kv,
    y_out,
    y_in,
    x_in,
    x_cut,
    gain_cut,
    inverse,
    norm_cut,
    token,
    sending,
    received,
    features,
    normed,
    deviation,
    project,
    encoder,
    load_sem,
    send_sem,
    recv_sem,
):
    me = lax.axis_index("seq")
    batch = lax.axis_index("batch")
    x = lax.rem(batch, 2)
    z, y, c = me // 4, lax.rem(me // 2, 2), lax.rem(me, 2)
    rows = q_in.shape[1]
    half = rows // 2
    lanes = 2 * GROUP * half
    shard = weight_ref.shape[0]
    scaling = HD ** (-0.5)
    factor = scaling * LOG2E

    up, down = {"seq": me + 4}, {"seq": me - 4}
    beside, core = {"seq": me + 2 - 4 * y}, {"seq": me + 1 - 2 * c}
    corner = {"seq": me + 2 - 4 * y + 1 - 2 * c}
    across = {"batch": batch + 1 - 2 * x}
    has_up, has_down = z < depth - 1, z > 0

    def far(k):
        return lax.rem(z + k, depth)

    def behind(k):
        return lax.rem(z + depth - k, depth)

    def plane(j):
        return {"seq": 4 * j + 2 * y + c}

    def head_at(ref, side, width):
        return ref.at[:, pl.ds(pl.multiple_of(side * width, 128), width)]

    def load(src, dst, index):
        copy = pltpu.make_async_copy(src, dst, load_sem.at[index])
        copy.start()
        return copy

    load_swap = [
        load(head_at(ref, 1 - y, HD), kv_swap.at[i], 6 + i)
        for i, ref in enumerate((keys_ref, values_ref))
    ]
    load_k = load(head_at(keys_ref, y, HD), k_all.at[z, c, y], 0)
    load_v = load(head_at(values_ref, y, HD), v_all.at[z, c, y], 1)
    load_w = load(weight_ref, w_all.at[z], 2)
    load_q = load(head_at(queries_ref, y, WIDE), q_in.at[y], 3)
    load_g = load(head_at(grads_ref, y, WIDE), g_in.at[y], 4)
    load_d = load(delta_hbm, d_in.at[y], 5)
    load_x = load(input_ref, x_in, 8)
    load_f = load(features_ref.at[0], features, 9)
    load_n = [load(gain_ref, gain_in, 13), load(post_ref, post_in, 14)]

    barrier = pltpu.get_barrier_semaphore()
    peers = [beside, core, corner, across] + [plane(far(k)) for k in range(1, depth)]
    for peer in peers:
        pl.semaphore_signal(barrier, inc=1, device_id=peer, device_id_type=MESH)
    pl.semaphore_wait(barrier, len(peers))

    copies = Copies(send_sem, recv_sem)

    over_y = copies.slots(5)
    for i, ref in enumerate((k_all, v_all)):
        load_swap[i].wait()
        copies.send(kv_swap.at[i], ref.at[z, c, y], over_y + i, beside)
    copies.send(head_at(queries_ref, 1 - y, WIDE), q_in.at[y], over_y + 2, beside)
    copies.send(head_at(grads_ref, 1 - y, WIDE), g_in.at[y], over_y + 3, beside)
    copies.send(delta_hbm, d_in.at[y], over_y + 4, beside)

    def spread(ref, load_own, swap):
        arrive = copies.slots(2 * depth)
        shared = copies.slots(2)

        def own(side, index):
            for k in range(depth - 1, 0, -1):
                copies.send(
                    ref.at[z, c, side], ref.at[z, c, side], arrive + 2 * k + index, plane(far(k))
                )
            copies.send(ref.at[z, c, side], ref.at[z, c, side], shared + index, core)

        def first():
            load_own.wait()
            own(y, 0)

        def second():
            copies.wait(ref.at[z, c, 1 - y], swap, beside)
            own(1 - y, 1)

        passed = copies.slots(depth)

        def relay():
            for k in range(1, depth):
                j = behind(k)
                for index in range(2):
                    side = y if index == 0 else 1 - y
                    copies.wait(ref.at[j, c, side], arrive + 2 * k + index, core)
                copies.send(ref.at[j, c], ref.at[j, c], passed + k, core)

        def finish():
            for index in range(2):
                side = y if index == 0 else 1 - y
                copies.wait(ref.at[z, 1 - c, side], shared + index, core)
            for k in range(1, depth):
                copies.wait(ref.at[behind(k), 1 - c], passed + k, core)

        return first, second, relay, finish

    k_first, k_second, k_relay, k_finish = spread(k_all, load_k, over_y)
    v_first, v_second, v_relay, v_finish = spread(v_all, load_v, over_y + 1)
    k_first()
    k_second()
    v_first()
    v_second()

    own_part = shard // 32 * 16
    between = shard - 2 * own_part
    pieces = split_rows(own_part, PIECES)

    def w_at(j, side, start, size):
        base = pl.multiple_of(side * (shard - own_part) + start, 16)
        return w_all.at[j, pl.ds(base, size)]

    def w_middle(j):
        return w_all.at[j, pl.ds(own_part, between)]

    count = len(pieces)
    w_recv = [copies.slots(depth) for _ in range(count + 1)]
    w_cross = [copies.slots(depth) for _ in range(count)]

    parts = list(range(count + (between > 0)))

    def w_send(j, upward, downward, some):
        for i in some:
            ref = w_at(j, x, *pieces[i]) if i < count else w_middle(j)
            if upward is not None:
                copies.send(ref, ref, w_recv[i] + j, up, upward)
            if downward is not None:
                copies.send(ref, ref, w_recv[i] + j, down, downward)

    def w_line(step, i):
        for j, present, upward in (
            (z - step, z - step >= 0, True),
            (z + step, z + step < depth, False),
        ):
            at = jnp.clip(j, 0, depth - 1)
            ref = w_at(at, x, *pieces[i]) if i < count else w_middle(at)
            yield at, present, upward, ref

    def w_take(step, i):
        for at, present, upward, ref in w_line(step, i):
            copies.wait(ref, w_recv[i] + at, core, present)
            if i < count:
                copies.send(ref, ref, w_cross[i] + at, across, present)

    def w_pass(step, i):
        if step == depth - 1:
            return
        for at, present, upward, ref in w_line(step, i):
            go = jnp.logical_and(present, has_up if upward else has_down)
            copies.send(ref, ref, w_recv[i] + at, up if upward else down, go)

    def w_relay(step, some):
        for i in some:
            w_take(step, i)
            w_pass(step, i)

    def w_finish(j, other):
        for i in range(count):
            copies.wait(w_at(j, 1 - x, *pieces[i]), w_cross[i] + j, across, other)

    load_w.wait()
    w_send(z, has_up, has_down, parts)

    def turned(device):
        return order_ref[2 * device] > order_ref[2 * device + 1]

    def arrange(source, target, side):
        flip = turned(4 * z + 2 * side + c)
        for h in range(GROUP):
            first = source[side, 0:half, h * HD : (h + 1) * HD]
            second = source[side, half:rows, h * HD : (h + 1) * HD]
            at = (side * GROUP + h) * half
            target[0, at : at + half] = jnp.where(flip, second, first)
            target[1, at : at + half] = jnp.where(flip, first, second)

    for copy in (load_q, load_g, load_d):
        copy.wait()
    k_relay()
    copies.wait(q_in.at[1 - y], over_y + 2, beside)
    for side in range(2):
        arrange(q_in, q_sort, side)

    def sort_keys(source, target):
        def one(index, carry):
            j, device = index // 4, lax.rem(index, 4)
            owner, side = device // 2, lax.rem(device, 2)
            flip = turned(4 * j + 2 * side + owner)
            first = source[j, owner, side, 0:half]
            second = source[j, owner, side, half:rows]
            at = pl.ds(pl.multiple_of(device * half, half), half)
            target[0, j, at] = jnp.where(flip, second, first)
            target[1, j, at] = jnp.where(flip, first, second)
            return carry

        lax.fori_loop(0, 4 * depth, one, 0)

    k_finish()
    sort_keys(k_all, k_sort)

    tiles = 3 * depth
    lane = lax.broadcasted_iota(jnp.int32, (1, lanes), 1)
    query_row = lax.rem(lane, half)
    in_first = lane < GROUP * half
    key_row = lax.broadcasted_iota(jnp.int32, (half, lanes), 0)

    def block_of(device, high):
        one, two = order_ref[2 * device], order_ref[2 * device + 1]
        return jnp.where(high == 1, jnp.maximum(one, two), jnp.minimum(one, two))

    def tile(t):
        kind, j = t // depth, lax.rem(t, depth)
        return j, kind // 2, (kind + 1) // 2

    top[...] = jnp.full_like(top, NEGATIVE)
    total[...] = jnp.zeros_like(total)
    acc[...] = jnp.zeros_like(acc)
    dq_acc[...] = jnp.zeros_like(dq_acc)

    def score_pass(t, carry):
        j, key_high, query_high = tile(t)
        score = lax.dot_general(
            k_sort[key_high, j],
            q_sort[query_high],
            (((1,), (1,)), ((), ())),
            preferred_element_type=jnp.float32,
        )
        query_blocks = [block_of(4 * z + 2 * side + c, query_high) for side in range(2)]
        best = top[query_high]
        for device in range(4):
            owner, side = device // 2, device % 2
            key_block = block_of(4 * j + 2 * side + owner, key_high)
            base, slope = [], []
            for query_block in query_blocks:
                live = (mask_ref[query_block, key_block] == 1) & (key_block <= query_block)
                same = live & (key_block == query_block)
                slope.append(same.astype(jnp.int32))
                base.append(jnp.where(same, 0, jnp.where(live, half, -1)))
            limit = jnp.where(in_first, base[0], base[1]) + query_row * jnp.where(
                in_first, slope[0], slope[1]
            )
            slab = score[device * half : (device + 1) * half]
            slab = jnp.where(key_row <= limit, slab, NEGATIVE)
            scores[t, device * half : (device + 1) * half] = slab
            best = jnp.maximum(best, jnp.max(slab.reshape(half // 8, 8, lanes), axis=0))
        top[query_high] = best
        return carry

    load_p = load(projector_ref, project, 12)
    lax.fori_loop(0, tiles, score_pass, 0)
    v_relay()
    for high in range(2):
        best = jnp.max(top[high], axis=0, keepdims=True)
        top[high] = jnp.broadcast_to(best * factor, (8, lanes))

    def sum_pass(t, carry):
        j, key_high, query_high = tile(t)
        peak = top[query_high][0:1]
        spread_out = jnp.exp2(scores[t] * factor - peak)
        total[query_high] += jnp.sum(spread_out.reshape(4 * half // 8, 8, lanes), axis=0)
        return carry

    lax.fori_loop(0, tiles, sum_pass, 0)
    for high in range(2):
        whole = jnp.sum(total[high], axis=0, keepdims=True)
        shift = top[high][0:1] + jnp.log2(whole)
        top[high] = jnp.broadcast_to(shift, (8, lanes))

    def spread_rows(line):
        return jnp.broadcast_to(line, (8, line.shape[1]))

    copies.wait(g_in.at[1 - y], over_y + 3, beside)
    copies.wait(d_in.at[1 - y], over_y + 4, beside)
    for side in range(2):
        arrange(g_in, g_sort, side)
        flip = turned(4 * z + 2 * side + c)
        for h in range(GROUP):
            line = jnp.where(y == 1, d_in[side, GROUP + h : GROUP + h + 1], d_in[side, h : h + 1])
            first, second = line[:, 0:half], line[:, half:rows]
            at = (side * GROUP + h) * half
            d_sort[0, :, at : at + half] = spread_rows(jnp.where(flip, second, first))
            d_sort[1, :, at : at + half] = spread_rows(jnp.where(flip, first, second))
    v_finish()
    sort_keys(v_all, v_sort)

    def grad_pass(t, carry):
        j, key_high, query_high = tile(t)
        prob = jnp.exp2(scores[t] * factor - top[query_high][0:1])
        grads = g_sort[query_high]
        prob_grad = lax.dot_general(
            v_sort[key_high, j], grads, (((1,), (1,)), ((), ())), preferred_element_type=jnp.float32
        )
        score_grad = (prob * (prob_grad - d_sort[query_high][0:1])).astype(jnp.bfloat16)
        acc[key_high, j, :, HD : 2 * HD] += jnp.dot(
            prob.astype(jnp.bfloat16), grads, preferred_element_type=jnp.float32
        )
        acc[key_high, j, :, 0:HD] += jnp.dot(
            score_grad, q_sort[query_high], preferred_element_type=jnp.float32
        )
        dq_acc[query_high] += lax.dot_general(
            k_sort[key_high, j],
            score_grad,
            (((0,), (0,)), ((), ())),
            preferred_element_type=jnp.float32,
        )
        return carry

    scale = jnp.where(
        lax.broadcasted_iota(jnp.int32, (half, 2 * HD), 1) < HD, jnp.float32(scaling), 1.0
    )

    def finish_part(j):
        for device in range(4):
            owner, side = device // 2, device % 2
            flip = turned(4 * j + 2 * side + owner)
            at = slice(device * half, (device + 1) * half)
            low, high = acc[0, j, at], acc[1, j, at]
            first = jnp.where(flip, high, low) * scale
            second = jnp.where(flip, low, high) * scale
            part[j, owner, side, 0:half] = first.astype(part.dtype)
            part[j, owner, side, half:rows] = second.astype(part.dtype)

    def wide(ref):
        return ref[...].astype(jnp.float32)

    by_core, by_plane = copies.slots(depth), copies.slots(depth)

    def add_cores(k):
        j = far(k)
        copies.wait(core_in.at[j], by_core + k, core)
        added = wide(part.at[j, c]) + wide(core_in.at[j])
        if k > 0:
            sum_out[k] = added.astype(sum_out.dtype)
            copies.send(sum_out.at[k], z_in.at[k], by_plane + k, plane(j))
        return added

    order = list(range(1, depth)) + [0]
    taken = 0
    for index, k in enumerate(order):
        j = far(k)
        lax.fori_loop(0, 3, lambda kind, carry: grad_pass(kind * depth + j, carry), 0)
        finish_part(j)
        copies.send(part.at[j, 1 - c], core_in.at[j], by_core + k, core)
        if index > 0:
            add_cores(order[index - 1])
        if index < len(parts) - 1:
            w_take(1, parts[index])
            taken = index + 1

    for high in range(2):
        q_turned = (jnp.transpose(dq_acc[high]) * scaling).astype(jnp.bfloat16)
        q_sort[high] = q_turned
    for side in range(2):
        flip = turned(4 * z + 2 * side + c)
        for h in range(GROUP):
            at = (side * GROUP + h) * half
            low, high = q_sort[0, at : at + half], q_sort[1, at : at + half]
            h_q[y, c, side, 0:half, h * HD : (h + 1) * HD] = jnp.where(flip, high, low)
            h_q[y, c, side, half:rows, h * HD : (h + 1) * HD] = jnp.where(flip, low, high)

    def quad_start(ref):
        first = copies.slots(3)
        here = ref.at[y, c]
        copies.send(here, here, first, beside)
        copies.send(here, here, first + 1, core)

        def relay():
            there = ref.at[1 - y, c]
            copies.wait(there, first, beside)
            copies.send(there, there, first + 2, core)

        def finish():
            copies.wait(ref.at[y, 1 - c], first + 1, core)
            copies.wait(ref.at[1 - y, 1 - c], first + 2, core)

        return relay, finish

    q_relay, q_finish = quad_start(h_q)
    summed = add_cores(0)
    for i in parts[taken:]:
        w_take(1, i)
    for i in parts:
        w_pass(1, i)

    width = 4 * shard
    model = depth * width
    for copy in [load_x, load_f] + load_n:
        copy.wait()
    gain = gain_in[...].reshape(1, model)
    squares = jnp.zeros((rows, 1), jnp.float32)
    for j in range(depth):
        block = x_in[:, j * width : (j + 1) * width]
        x_cut[j] = block
        block = block.astype(jnp.float32)
        squares += jnp.sum(block * block, axis=1, keepdims=True)
        gain_cut[j] = jnp.broadcast_to(
            gain[:, j * width : (j + 1) * width], (8, width)
        )
    inverse[...] = jnp.broadcast_to(lax.rsqrt(squares / model + EPSILON), inverse.shape)
    seen = features[...].astype(jnp.float32)
    centered = seen - jnp.mean(seen, axis=1, keepdims=True)
    spread_of = lax.rsqrt(jnp.mean(centered * centered, axis=1, keepdims=True) + EPSILON)
    normed[...] = centered * spread_of
    deviation[...] = jnp.broadcast_to(spread_of, deviation.shape)

    for k in range(1, depth):
        copies.wait(z_in.at[k], by_plane + k, core)
        summed = summed + wide(z_in.at[k])
    h_kv[y, c] = summed.astype(h_kv.dtype)
    kv_relay, kv_finish = quad_start(h_kv)
    near = list(range(2, depth - 1))
    for step in near[:-1]:
        w_relay(step, parts)
    cuts = [len(parts) * i // 4 for i in range(5)]
    groups = [parts[a:b] for a, b in zip(cuts, cuts[1:])]

    def w_some(index):
        if near:
            w_relay(near[-1], groups[index])

    w_some(0)
    q_relay()
    w_some(1)
    w_some(2)
    kv_relay()
    q_finish()
    kv_finish()

    heads = jnp.concatenate(
        [h_q[g].reshape(4 * rows, WIDE) for g in range(KVH)]
        + [
            h_kv[g, :, :, :, part_of * HD : (part_of + 1) * HD].reshape(4 * rows, HD)
            for part_of in range(2)
            for g in range(KVH)
        ],
        axis=1,
    )
    step_of = jnp.where(2 * z >= depth, depth - 1, 1)
    mine = 2 * y + c
    y_recv = copies.slots(4 * depth)

    def multiply(k):
        j = lax.rem(z + k * step_of, depth)
        if k > 0:
            w_finish(j, None)
        block = lax.dot_general(
            heads, w_all[j], (((1,), (1,)), ((), ())), preferred_element_type=jnp.float32
        )
        y_out[j] = block.astype(y_out.dtype).reshape(2, 2, rows, shard)
        for device, owner, side in (
            (beside, c, 1 - y),
            (corner, 1 - c, 1 - y),
            (core, 1 - c, y),
        ):
            copies.send(
                y_out.at[j, owner, side], y_in.at[j, mine], y_recv + 4 * j + mine, device
            )

    def collect(k, dots):
        j = lax.rem(z + k * step_of, depth)
        for source, device in (
            (2 * y + 1 - c, core),
            (2 * (1 - y) + c, beside),
            (2 * (1 - y) + 1 - c, corner),
        ):
            copies.wait(y_in.at[j, source], y_recv + 4 * j + source, device)
        y_in[j, mine] = y_out[j, c, y]
        block = jnp.concatenate([wide(y_in.at[j, source]) for source in range(4)], axis=1)
        block = block * gain_cut[j][0:1]
        norm_cut[j] = block
        return dots + jnp.sum(block * x_cut[j].astype(jnp.float32), axis=1, keepdims=True)

    dots = jnp.zeros((rows, 1), jnp.float32)
    for k in range(depth - 1):
        if k == depth - 2:
            w_relay(depth - 1, groups[0])
            w_relay(depth - 1, groups[1])
        multiply(k)
        if k == 0:
            w_some(3)
    w_relay(depth - 1, groups[2])
    dots = collect(0, dots)
    w_relay(depth - 1, groups[3])
    for k in range(1, depth - 1):
        dots = collect(k, dots)
    multiply(depth - 1)
    dots = collect(depth - 1, dots)

    scale_in = inverse[:, 0:1]
    pull = scale_in * scale_in * scale_in * (dots / model)
    for j in range(depth):
        block = scale_in * norm_cut[j] - x_cut[j].astype(jnp.float32) * pull
        token[:, j * width : (j + 1) * width] = block.astype(token.dtype)

    start = jnp.int32(0)
    for frame in range(owner_ref.shape[0]):
        start = start + jnp.where(owner_ref[frame] == me, 2 * frame, 0)
    one, two = order_ref[2 * me], order_ref[2 * me + 1]
    keep_first = (one == start) | (one == start + 1)
    leading = jnp.where(keep_first, one, two) == start
    sending[...] = jnp.where(keep_first, token[half:rows], token[0:half])
    frame_recv = copies.slots(1)
    copies.send(sending, received, frame_recv, core)
    store_token = pltpu.make_async_copy(token, token_ref, load_sem.at[10])
    store_token.start()
    load_p.wait()
    kept = jnp.where(keep_first, token[0:half], token[half:rows])
    copies.wait(received, frame_recv, core)
    other = received[...]
    frame = jnp.concatenate(
        [jnp.where(leading, kept, other), jnp.where(leading, other, kept)], axis=0
    )
    post = lax.dot_general(
        frame, project[...], (((1,), (1,)), ((), ())), preferred_element_type=jnp.float32
    )
    post = post * post_in[...].reshape(1, post.shape[1])
    flat = normed[...]
    post = (
        post
        - jnp.mean(post, axis=1, keepdims=True)
        - flat * jnp.mean(post * flat, axis=1, keepdims=True)
    )
    encoder[...] = (deviation[:, 0:1] * post).astype(encoder.dtype)
    store_encoder = pltpu.make_async_copy(encoder, encoder_ref.at[0], load_sem.at[11])
    store_encoder.start()
    copies.drain()
    counts.append((copies.sends, copies.recvs))
    store_token.wait()
    store_encoder.wait()


def hand_over_kernel(token_ref, encoder_ref, token_out, encoder_out, token, encoder, sem):
    rows = token.shape[0] // CUTS
    moves = [
        (token_ref.at[at], token_out.at[at], token.at[at])
        for at in (pl.ds(i * rows, rows) for i in range(CUTS))
    ] + [(encoder_ref, encoder_out, encoder)]
    loads, stores = [], []
    for i, (source, target, buffer) in enumerate(moves):
        loads.append(pltpu.make_async_copy(source, buffer, sem.at[0, i]))
        stores.append(pltpu.make_async_copy(buffer, target, sem.at[1, i]))
    for copy in loads:
        copy.start()
    for copy_in, copy_out in zip(loads, stores):
        copy_in.wait()
        copy_out.start()
    for copy in stores:
        copy.wait()


def hand_over(token, encoder):
    anywhere = pl.BlockSpec(memory_space=pl.ANY)
    return pl.pallas_call(
        hand_over_kernel,
        out_shape=tuple(jax.ShapeDtypeStruct(a.shape, a.dtype) for a in (token, encoder)),
        in_specs=[anywhere, anywhere],
        out_specs=(anywhere, anywhere),
        scratch_shapes=[
            pltpu.VMEM(token.shape, token.dtype),
            pltpu.VMEM(encoder.shape, encoder.dtype),
            pltpu.SemaphoreType.DMA((2, CUTS + 1)),
        ],
        name="hand_over",
    )(token, encoder)


def layer_grads(arguments, count):
    (
        order,
        mask,
        queries,
        out_grad,
        row_delta,
        keys,
        values,
        weight,
        layer_input,
        norm_gain,
        frame_owner,
        features,
        post_gain,
        projector,
    ) = arguments
    depth = count // 4
    rows = queries.shape[0]
    half = rows // 2
    lanes = 2 * GROUP * half
    shard, qkv = weight.shape
    low, wide = jnp.bfloat16, jnp.float32
    smem = pl.BlockSpec(memory_space=pltpu.SMEM)
    vmem = pl.BlockSpec(memory_space=pltpu.VMEM)
    anywhere = pl.BlockSpec(memory_space=pl.ANY)
    kv_shape = (depth, 2, 2, rows, HD)
    pair = (2, rows, 2 * HD)
    def build(counts, sends, recvs):
        return pl.pallas_call(
        functools.partial(layer_kernel, depth, counts),
        out_shape=(
            jax.ShapeDtypeStruct(layer_input.shape, low),
            jax.ShapeDtypeStruct(features.shape, low),
        ),
        in_specs=[smem, smem] + [anywhere] * 7 + [anywhere, smem, anywhere, anywhere, anywhere],
        out_specs=(anywhere, anywhere),
        scratch_shapes=[
            pltpu.VMEM(norm_gain.shape, wide),
            pltpu.VMEM(post_gain.shape, wide),
            pltpu.VMEM((2, rows, HD), low),
            pltpu.VMEM(kv_shape, low),
            pltpu.VMEM(kv_shape, low),
            pltpu.VMEM((2, rows, WIDE), low),
            pltpu.VMEM((2, rows, WIDE), low),
            pltpu.VMEM((2,) + row_delta.shape, wide),
            pltpu.VMEM((depth, shard, qkv), low),
            pltpu.VMEM((2, depth, 4 * half, HD), low),
            pltpu.VMEM((2, depth, 4 * half, HD), low),
            pltpu.VMEM((2, lanes, HD), low),
            pltpu.VMEM((2, lanes, HD), low),
            pltpu.VMEM((2, 8, lanes), wide),
            pltpu.VMEM((3 * depth, 4 * half, lanes), wide),
            pltpu.VMEM((2, 8, lanes), wide),
            pltpu.VMEM((2, 8, lanes), wide),
            pltpu.VMEM((2, HD, lanes), wide),
            pltpu.VMEM((2, depth, 4 * half, 2 * HD), wide),
            pltpu.VMEM((depth, 2) + pair, low),
            pltpu.VMEM((depth,) + pair, low),
            pltpu.VMEM((depth,) + pair, low),
            pltpu.VMEM((depth,) + pair, low),
            pltpu.VMEM((2, 2, 2, rows, WIDE), low),
            pltpu.VMEM((2, 2, 2, rows, 2 * HD), low),
            pltpu.VMEM((depth, 2, 2, rows, shard), low),
            pltpu.VMEM((depth, 4, rows, shard), low),
            pltpu.VMEM(layer_input.shape, low),
            pltpu.VMEM((depth, rows, 4 * shard), low),
            pltpu.VMEM((depth, 8, 4 * shard), wide),
            pltpu.VMEM((rows, 128), wide),
            pltpu.VMEM((depth, rows, 4 * shard), wide),
            pltpu.VMEM(layer_input.shape, low),
            pltpu.VMEM((half, layer_input.shape[1]), low),
            pltpu.VMEM((half, layer_input.shape[1]), low),
            pltpu.VMEM(features.shape[1:], low),
            pltpu.VMEM(features.shape[1:], wide),
            pltpu.VMEM((rows, 128), wide),
            pltpu.VMEM(projector.shape, low),
            pltpu.VMEM(features.shape[1:], low),
            pltpu.SemaphoreType.DMA((15,)),
            pltpu.SemaphoreType.DMA((sends,)),
            pltpu.SemaphoreType.DMA((recvs,)),
        ],
        compiler_params=pltpu.CompilerParams(
            collective_id=0, has_side_effects=True, vmem_limit_bytes=67043328
        ),
        name="layer_grads",
    )

    counts = []
    jax.eval_shape(build(counts, 4096, 4096), *arguments)
    return build([], *counts[0])(*arguments)


def body(
    queries,
    keys,
    values,
    out_grad,
    row_delta,
    layer_input,
    norm_gain,
    qkv_weight,
    block_order,
    block_mask,
    frame_owner,
    vision_features,
    post_gain,
    projector,
):
    arguments = (
        block_order,
        block_mask,
        queries,
        out_grad,
        row_delta.T,
        keys,
        values,
        qkv_weight,
        layer_input,
        norm_gain,
        frame_owner,
        vision_features,
        post_gain,
        projector,
    )
    return hand_over(*layer_grads(arguments, lax.axis_size("seq")))


def solution(mesh):
    placed = (
        P(("batch", "seq"), None),
        P(("batch", "seq"), None),
        P(("batch", "seq"), None),
        P(("batch", "seq"), None),
        P(("batch", "seq"), None),
        P(("batch", "seq"), None),
        P(),
        P("seq", None),
        P("batch"),
        P("batch", None),
        P("batch"),
        P(("batch", "seq"), None, None),
        P(),
        P(),
    )
    return jax.shard_map(
        body,
        mesh=mesh,
        in_specs=placed,
        out_specs=(P(("batch", "seq"), None), P(("batch", "seq"), None, None)),
        check_vma=False,
    )
```
